256 devices in a mesh: grp: 2 (over z), slab: 128 (over y, x, core).
Axes of the slice: x: 8, y: 8, z: 2, core: 2. Of those that a mesh axis runs over, the one named last changes fastest.
The devices are a block of a 8x8x16 slice.
Arguments:
- volume: bfloat16 [512, 1024, 1024], P(('grp', 'slab')), parts along dimension 0, may hold values from -60 to 60
- plane_shift: int32 [4, 256], P('grp', 'slab'), parts along dimension 0, may hold values from -64 to 64
- plane_weight: float32 [4, 256], P('grp', 'slab'), parts along dimension 0, may hold values from 0 to 1
- column_left: int32 [4, 1024], P('grp'), parts along dimension 0, may hold values from 0 to 1022
- column_weight: float32 [4, 1024], P('grp'), parts along dimension 0, may hold values from 0 to 1
- window_center: int32 [4, 2], P('grp'), parts along dimension 0, may hold values from -200 to 199
- tilt_owner: int32 [256], P('grp'), parts along dimension 0, may hold values from 0 to 127, each once
- reference_band: float32 [256, 2, 128, 128], P(('grp', 'slab')), parts along dimension 0, may hold values from -6 to 6
Outputs:
- correlation: float32 [4, 128, 128], P('grp', 'slab'), parts along dimension 0
- peaks: float32 [4], P('grp'), parts along dimension 0
The draws below stay inside these ranges and needn't reach their ends.
There are 2 independent parts, one for each index of `grp`. The reference program is written for one: setup_inputs(seed, part) draws one part's arguments, and reference() takes and returns one part's arrays. A program takes and returns all parts, laid end to end along the dimension named above; each array names one. Nothing has to cross between parts.
Inputs may be any that keep to these rules, and one draw needn't show every extreme that they name: `tilt_owner`: the first 2 entries name the owners of the tilts, one slab index each.
All inputs are finite; a program needn't handle non-finite values.
Results may differ from the reference program's by a relative error of at most 0.0003.
Values sent between devices are 32-bit elements; how exact they have to be, the bound alone decides.
No kernel may reach another device: no remote copies, remote signals or barrier semaphores. Data moves between devices by JAX's collectives and lax.ppermute only.
A program may use at most 128 MiB of HBM per device.

```python
import math
import jax
import jax.numpy as jnp
from jax import lax

Y = 1024
X = 1024
BAND = 128
WIN_COLS = 128
TILTS = 2
PLANES = 256
WIN_ROWS = 128
N_SLAB = 128


def draw_volume(key, part):
    first_key, second_key, third_key = jax.random.split(key, 3)
    col_scale = jnp.exp(jax.random.uniform(second_key, (1, 1, X), jnp.float32) * math.log(10.0))
    row_scale = jnp.exp(jax.random.uniform(third_key, (1, Y, 1), jnp.float32) * math.log(10.0))
    base = jnp.clip(jax.random.normal(first_key, (PLANES, Y, X), jnp.float32), -6.0, 6.0)
    return (base * col_scale * row_scale / 10.0).astype(jnp.bfloat16)


def set_ends(values, own_key, smallest, high):
    dims = values.shape
    place = [jax.random.randint(jax.random.fold_in(own_key, axis), (), 0, dims[axis]) for axis in range(len(dims))]
    values = values.at[tuple(place)].set(smallest)
    longest = dims.index(max(dims))
    place[longest] = (place[longest] + 1) % dims[longest]
    return values.at[tuple(place)].set(high)


def level_of(key, extent, pieces, least, largest):
    factor_of = 1.0
    for dim, shards_of in pieces:
        draws = jax.random.uniform(jax.random.fold_in(jax.random.fold_in(key, 6), dim), (shards_of,), jnp.float32, least / len(pieces), largest / len(pieces))
        factor_of = factor_of * jnp.repeat(jnp.exp(draws), extent[dim] // shards_of).reshape((-1,) + (1,) * (len(extent) - 1 - dim))
    return factor_of


def gaussian(own_key, extent, spread, most, cuts=(), kind=jnp.bfloat16):
    result = jax.random.normal(own_key, extent, jnp.float32) * spread
    if len(cuts) > 0:
        result = level_of(own_key, extent, cuts, -0.22, 0.18) * result
    return jnp.clip(result, min=-most, max=most).astype(kind)


def setup_inputs(seed: int = 0, part: int = 0) -> dict:
    seeds = jax.random.split(jax.random.key(seed), 9)
    own_keys = jax.random.split(jax.random.fold_in(seeds[8], part), 9)
    volume = draw_volume(jax.random.fold_in(jax.random.fold_in(seeds[8], part), 71), part)
    plane_shift = set_ends(jax.random.randint(own_keys[1], (TILTS, PLANES), -(X // 16), X // 16 + 1), jax.random.fold_in(own_keys[1], 1), -(X // 16), (X // 16 + 1) - 1).astype(jnp.int32)
    plane_weight = jnp.clip(1.0 * jax.random.uniform(own_keys[2], (TILTS, PLANES), jnp.float32) ** level_of(own_keys[2], (TILTS, PLANES), ((1, 128),), -0.2, 0.2), 0.0, 1.0)
    column_left = set_ends(jax.random.randint(own_keys[3], (TILTS, X), 0, X - 1), jax.random.fold_in(own_keys[3], 1), 0, (X - 1) - 1).astype(jnp.int32)
    column_weight = jnp.clip(jax.random.uniform(own_keys[4], (TILTS, X), jnp.float32, 0.0, 1.0), 0.0, 1.0)
    window_center = set_ends(jax.random.randint(own_keys[5], (TILTS, 2), -200, 200), jax.random.fold_in(own_keys[5], 1), -200, 199).astype(jnp.int32)
    tilt_owner = jax.random.permutation(own_keys[6], N_SLAB).astype(jnp.int32)
    reference_band = gaussian(own_keys[7], (N_SLAB, 2, BAND, BAND), 1.0, 6.0, ((0, 128),), jnp.float32)
    return {"volume": volume, "plane_shift": plane_shift, "plane_weight": plane_weight, "column_left": column_left, "column_weight": column_weight, "window_center": window_center, "tilt_owner": tilt_owner, "reference_band": reference_band}


def project_tilt(volume, shift_row, weight_row, left_row, share_row):
    margin = X // 16 + 1

    def add_plane(total, items):
        plane_data, shift_value, weight_value = items
        padded = jnp.pad(plane_data.astype(jnp.float32), ((0, 0), (margin, margin)))
        near_cells = lax.dynamic_slice_in_dim(padded, (margin - shift_value).astype(jnp.int32), X, 1)
        far_cells = lax.dynamic_slice_in_dim(padded, (margin - shift_value - 1).astype(jnp.int32), X, 1)
        return (total + (1.0 - weight_value) * near_cells + weight_value * far_cells, None)
    summed, _ = lax.scan(add_plane, jnp.zeros((Y, X), jnp.float32), (volume, shift_row, weight_row))
    left_values = jnp.take(summed, left_row, axis=1)
    right_values = jnp.take(summed, left_row + 1, axis=1)
    return (1.0 - share_row) * left_values + share_row * right_values

def phase_pair(left_ints, right_ints, length):
    product = left_ints[:, None] * right_ints[None, :] % length
    angle = product.astype(jnp.float32) * (2.0 * math.pi / length)
    return (jnp.cos(angle), jnp.sin(angle))

def matmul(first, second):
    return jnp.dot(first, second, precision=lax.Precision.HIGHEST, preferred_element_type=jnp.float32)

def reference(volume, plane_shift, plane_weight, column_left, column_weight, window_center, tilt_owner, reference_band):
    freq_cols = jnp.arange(BAND, dtype=jnp.int32)
    freq_rows = freq_cols - BAND // 2
    band_rows = freq_rows % Y
    outputs = []
    maxima = []
    for which in range(TILTS):
        projected = project_tilt(volume, plane_shift[which], plane_weight[which], column_left[which], column_weight[which])
        full_spec = jnp.fft.fft2(projected)
        band_spec = jnp.take(full_spec, band_rows, axis=0)[:, :BAND]
        spec_real = jnp.real(band_spec).astype(jnp.float32)
        spec_imag = jnp.imag(band_spec).astype(jnp.float32)
        owned = reference_band[tilt_owner[which]]
        ref_real, ref_imag = (owned[0], owned[1])
        cross_real = spec_real * ref_real + spec_imag * ref_imag
        cross_imag = spec_imag * ref_real - spec_real * ref_imag
        energy_spec = jnp.mean(spec_real * spec_real + spec_imag * spec_imag) + 1e-06
        energy_ref = jnp.mean(ref_real * ref_real + ref_imag * ref_imag) + 1e-06
        offsets_y = window_center[which, 0] + jnp.arange(WIN_ROWS, dtype=jnp.int32) - WIN_ROWS // 2
        offsets_x = window_center[which, 1] + jnp.arange(WIN_COLS, dtype=jnp.int32) - WIN_COLS // 2
        row_cos, row_sin = phase_pair(offsets_y, freq_rows, Y)
        col_cos, col_sin = phase_pair(freq_cols, offsets_x, X)
        half_real = matmul(row_cos, cross_real) - matmul(row_sin, cross_imag)
        half_imag = matmul(row_cos, cross_imag) + matmul(row_sin, cross_real)
        corr = (matmul(half_real, col_cos) - matmul(half_imag, col_sin)) / (BAND * jnp.sqrt(energy_spec * energy_ref))
        outputs.append(corr)
        maxima.append(jnp.max(corr))
    return (jnp.stack(outputs), jnp.stack(maxima))
```

```python
import numpy as np

import jax
import jax.numpy as jnp
from jax import lax
from jax.experimental import pallas as pl
from jax.experimental.pallas import tpu as pltpu
from jax.sharding import Mesh, PartitionSpec as P
import ml_dtypes

BAND = 128
HALF = BAND // 2
WIN = 128
TILTS = 2
INNER = 16
PAIRS = HALF // INNER
ROWS = 136
LANES = 128
CH_IN = 12 * PAIRS
CH_MID = 16 * PAIRS
CH_OUT = 24


def split(table):
    table = np.asarray(table, np.float32)
    high = table.astype(ml_dtypes.bfloat16)
    low = (table - high.astype(np.float32)).astype(ml_dtypes.bfloat16)
    return high, low


def turns(a, b, length):
    angle = (a[:, None].astype(np.int64) * b[None, :]) % length * (2.0 * np.pi / length)
    return np.cos(angle), np.sin(angle)


def row_table(length):
    c, s = turns(np.arange(HALF + 1), np.arange(length), length)
    out = np.zeros((ROWS, length))
    out[:HALF] = c[:HALF]
    out[HALF] = c[HALF]
    out[HALF + 1 : BAND] = s[1:HALF]
    out[BAND] = s[HALF]
    high, low = split(out)
    return np.concatenate([high, low])


def column_table(length):
    c, s = turns(np.arange(length), np.arange(BAND), length)
    high, low = split(np.concatenate([c, s], 1))
    return np.stack([high, low])


def window_column_table(length):
    c, s = turns(np.arange(BAND), np.arange(WIN) - WIN // 2, length)
    high, low = split(np.concatenate([c, -s], 0))
    return np.stack([high, low])


def window_row_table(length):
    c, s = turns(np.arange(WIN) - WIN // 2, np.arange(HALF + 1), length)
    out = np.zeros((TILTS, WIN, INNER, CH_OUT))
    for t in range(TILTS):
        for k in range(INNER):
            for r in range(PAIRS):
                p = k * PAIRS + r
                out[t, :, k, 2 * PAIRS * t + r] = c[:, p]
                out[t, :, k, 2 * PAIRS * t + PAIRS + r] = -s[:, p] if p else c[:, HALF]
        out[t, :, 0, 4 * PAIRS + t] = s[:, HALF]
    high, low = split(out.reshape(TILTS * WIN, INNER * CH_OUT))
    return np.stack([high, low])


def dot(a, b):
    return jnp.dot(a, b, preferred_element_type=jnp.float32)


def halves(x):
    high = x.astype(jnp.bfloat16)
    return high, (x - high.astype(jnp.float32)).astype(jnp.bfloat16)


def spectrum_kernel(shift, weight, volume, row_tab, col_tab, left, share, ref, out, rpad, sums, lhs, proj, band):
    planes, height, width = volume.shape
    tiles = width // LANES
    step = 256
    rpad[:, :, :LANES] = jnp.zeros((planes, ROWS, LANES), jnp.float32)
    rpad[:, :, LANES + width :] = jnp.zeros((planes, ROWS, LANES), jnp.float32)
    for z in range(planes):
        for n in range(0, width, step):
            r = dot(row_tab[...], volume[z, :, n : n + step])
            rpad[z, :, LANES + n : LANES + n + step] = r[:ROWS] + r[ROWS:]
    lane = lax.broadcasted_iota(jnp.int32, (8, LANES), 1)
    for t in range(TILTS):

        def shift_rows(g, _, t=t):
            rows = pl.ds(pl.multiple_of(g * 8, 8), 8)
            total = [None] * tiles
            for z in range(planes):
                w = weight[t, z]
                for more, factor in ((0, 1.0 - w), (1, w)):
                    s = shift[t, z] + more
                    off = jnp.where(s < 0, 1, 0)
                    turn = jnp.where(s < 0, s + LANES, s)
                    mask = lane < turn
                    turned = []
                    for j in range(tiles + 1):
                        at = pl.multiple_of((j + off) * LANES, LANES)
                        turned.append(pltpu.roll(rpad[z, rows, pl.ds(at, LANES)], turn, 1))
                    for j in range(tiles):
                        term = factor * jnp.where(mask, turned[j], turned[j + 1])
                        total[j] = term if total[j] is None else total[j] + term
            for j in range(tiles):
                sums[rows, j * LANES : (j + 1) * LANES] = total[j]
            return 0

        lax.fori_loop(0, ROWS // 8, shift_rows, 0)
        here = sums[:ROWS, :]
        sums[ROWS:, :] = pltpu.roll(here, width - 1, 1)
        high, low = halves(sums[...])
        lhs[: 2 * ROWS] = high
        lhs[2 * ROWS :] = low
        place = lax.broadcasted_iota(jnp.int32, (width, step), 0)
        for n in range(0, width, step):
            pick = jnp.where(place == left[t : t + 1, n : n + step], 1.0, 0.0).astype(jnp.bfloat16)
            y = dot(lhs[...], pick)
            y = y[: 2 * ROWS] + y[2 * ROWS :]
            cw = share[t : t + 1, n : n + step]
            proj[t * ROWS : (t + 1) * ROWS, n : n + step] = (1.0 - cw) * y[:ROWS] + cw * y[ROWS:]
    high, low = halves(proj[...])
    band[...] = dot(high, col_tab[0]) + dot(low, col_tab[0]) + dot(high, col_tab[1])
    for t in range(TILTS):
        b = t * ROWS
        row = band[b + HALF : b + HALF + 1, :]
        last = band[b + BAND : b + BAND + 1, :]
        band[b + HALF : b + HALF + 1, :BAND] = row[:, :BAND] + last[:, BAND:]
        band[b + HALF : b + HALF + 1, BAND:] = row[:, BAND:] - last[:, :BAND]
    for k in range(INNER):
        for t in range(TILTS):
            for i, (r0, c0) in enumerate(((0, 0), (0, BAND), (HALF, 0), (HALF, BAND))):
                at = t * ROWS + r0 + k * PAIRS
                to = (4 * t + i) * PAIRS
                out[k, to : to + PAIRS, :] = band[at : at + PAIRS, c0 : c0 + BAND]
        for i in range(2):
            to = (8 + i) * PAIRS
            a = HALF + k * PAIRS
            out[k, to : to + PAIRS, :] = ref[0, i, a : a + PAIRS, :]
            for r in range(PAIRS):
                p = k * PAIRS + r
                a = HALF - p if p else 0
                to = (10 + i) * PAIRS + r
                out[k, to : to + 1, :] = ref[0, i, a : a + 1, :]


def row_sum_kernel(info, got, out):
    n = got.shape[0]
    mine = info[0]
    total = got[0, : 8 * PAIRS, :]
    for s in range(1, n):
        total = total + got[s, : 8 * PAIRS, :]
    refs = []
    for t in range(TILTS):
        owner = info[1 + t]
        piece = got[lax.rem(owner, n), 8 * PAIRS :, :]
        refs.append(jnp.where(lax.div(owner, n) == mine, piece, 0.0))
    for y in range(out.shape[0]):
        out[y, : 8 * PAIRS, :] = total
        for t in range(TILTS):
            out[y, (8 + 4 * t) * PAIRS : (12 + 4 * t) * PAIRS, :] = refs[t]


def cross_kernel(length, info, center, got, tab, out, lhs):
    n = got.shape[0]
    total = got[0]
    for s in range(1, n):
        total = total + got[s]
    k = info[0]
    b = lax.broadcasted_iota(jnp.int32, (PAIRS, BAND), 1)
    p = k * PAIRS + lax.broadcasted_iota(jnp.int32, (PAIRS, BAND), 0)
    zero = p == 0
    lhs[...] = jnp.zeros(lhs.shape, jnp.float32)
    energies = []
    for t in range(TILTS):

        def part(i):
            return total[i * PAIRS : (i + 1) * PAIRS, :]

        cc, cs, sc, ss = (part(4 * t + i) for i in range(4))
        refs = [part(8 + 4 * t + i) for i in range(4)]
        plus = (jnp.where(zero, cc, cc - ss), -jnp.where(zero, cs, cs + sc))
        minus = (jnp.where(zero, sc, cc + ss), -jnp.where(zero, ss, cs - sc))
        crossed = []
        e_spec = e_ref = 0.0
        for (sr, si), (rr, ri), q in ((plus, refs[:2], p), (minus, refs[2:], jnp.where(zero, -HALF, -p))):
            cr = sr * rr + si * ri
            ci = si * rr - sr * ri
            e_spec = e_spec + sr * sr + si * si
            e_ref = e_ref + rr * rr + ri * ri
            angle = ((q * center[t, 0] + b * center[t, 1]) & (length - 1)).astype(jnp.float32) * (2.0 * np.pi / length)
            co, si_ = jnp.cos(angle), jnp.sin(angle)
            crossed.append((cr * co - ci * si_, cr * si_ + ci * co))
        (pr, pi), (mr, mi) = crossed
        at = 2 * PAIRS * t
        lhs[at : at + PAIRS, :BAND] = jnp.where(zero, pr, pr + mr)
        lhs[at : at + PAIRS, BAND:] = jnp.where(zero, pi, pi + mi)
        lhs[at + PAIRS : at + 2 * PAIRS, :BAND] = jnp.where(zero, mr, pi - mi)
        lhs[at + PAIRS : at + 2 * PAIRS, BAND:] = jnp.where(zero, mi, mr - pr)
        extra = 4 * PAIRS + t
        lhs[extra : extra + 1, :BAND] = mi[:1]
        lhs[extra : extra + 1, BAND:] = -mr[:1]
        energies += [jnp.sum(e_spec, 0, keepdims=True), jnp.sum(e_ref, 0, keepdims=True)]
    high, low = halves(lhs[...])
    h = dot(high, tab[0]) + dot(low, tab[0]) + dot(high, tab[1])
    h = h[:CH_OUT]
    for d in range(out.shape[0]):
        out[d] = h
        for i, e in enumerate(energies):
            to = 4 * PAIRS + TILTS + i
            out[d, to : to + 1, :] = e


def window_kernel(info, got, tab, rows, peaks, corr):
    x = got[...].reshape(got.shape[0] * CH_OUT, WIN)
    high, low = halves(x)
    c = dot(tab[0], high) + dot(tab[0], low) + dot(tab[1], high)
    e = jnp.sum(jnp.sum(got[:, 4 * PAIRS + TILTS :, :], 0), 1, keepdims=True)
    for t in range(TILTS):
        spec = e[2 * t : 2 * t + 1] / (BAND * BAND) + 1e-06
        ref = e[2 * t + 1 : 2 * t + 2] / (BAND * BAND) + 1e-06
        mine = c[t * WIN : (t + 1) * WIN] / (BAND * jnp.sqrt(spec * ref))
        corr[t] = mine
        peaks[t] = jnp.max(mine)
        rows[t] = corr[t, pl.ds(info[0], 1), :]


def solution(mesh):
    outer = mesh.shape["slab"] // INNER
    grid = Mesh(
        mesh.devices.reshape(mesh.shape["grp"], outer, INNER), ("grp", "line", "seat")
    )
    slab = ("line", "seat")
    vmem = pl.BlockSpec(memory_space=pltpu.VMEM)
    smem = pl.BlockSpec(memory_space=pltpu.SMEM)
    big = pltpu.CompilerParams(vmem_limit_bytes=48 * 1024 * 1024)

    def per_device(volume, shift, weight, left, share, center, owner, ref):
        planes, height, width = volume.shape
        line = lax.axis_index("line")
        seat = lax.axis_index("seat")
        f32 = jnp.float32
        packed = pl.pallas_call(
            spectrum_kernel,
            out_shape=jax.ShapeDtypeStruct((INNER, CH_IN, BAND), f32),
            in_specs=[smem, smem] + [vmem] * 6,
            out_specs=vmem,
            scratch_shapes=[
                pltpu.VMEM((planes, ROWS, width + 2 * LANES), f32),
                pltpu.VMEM((2 * ROWS, width), f32),
                pltpu.VMEM((4 * ROWS, width), jnp.bfloat16),
                pltpu.VMEM((TILTS * ROWS, width), f32),
                pltpu.VMEM((TILTS * ROWS, 2 * BAND), f32),
            ],
            compiler_params=big,
            name="spectrum",
        )(shift, weight, volume, jnp.asarray(row_table(height)), jnp.asarray(column_table(width)), left, share, ref)
        got = lax.all_to_all(packed, "seat", 0, 0, tiled=True)
        info = jnp.concatenate([line[None], owner[:TILTS]]).astype(jnp.int32)
        summed = pl.pallas_call(
            row_sum_kernel,
            out_shape=jax.ShapeDtypeStruct((outer, CH_MID, BAND), f32),
            in_specs=[smem, vmem],
            out_specs=vmem,
            name="row_sum",
        )(info, got)
        got = lax.all_to_all(summed, "line", 0, 0, tiled=True)

        def cross(*refs):
            cross_kernel(width, *refs)

        piece = pl.pallas_call(
            cross,
            out_shape=jax.ShapeDtypeStruct((INNER, CH_OUT, WIN), f32),
            in_specs=[smem, smem, vmem, vmem],
            out_specs=vmem,
            scratch_shapes=[pltpu.VMEM((32, 2 * BAND), f32)],
            name="cross",
        )(seat[None].astype(jnp.int32), center, got, jnp.asarray(window_column_table(width)))
        got = lax.all_to_all(piece, "seat", 0, 0, tiled=True)
        rows, peaks = pl.pallas_call(
            window_kernel,
            out_shape=[jax.ShapeDtypeStruct((TILTS, 1, WIN), f32), jax.ShapeDtypeStruct((TILTS,), f32)],
            in_specs=[smem, vmem, vmem],
            out_specs=[vmem, smem],
            scratch_shapes=[pltpu.VMEM((TILTS, WIN, WIN), f32)],
            name="window",
        )((line * INNER + seat)[None].astype(jnp.int32), got, jnp.asarray(window_row_table(height)))
        return rows, peaks

    placed = (
        P(("grp",) + slab, None, None),
        P("grp", slab),
        P("grp", slab),
        P("grp", None),
        P("grp", None),
        P("grp", None),
        P("grp"),
        P(("grp",) + slab, None, None, None),
    )
    return jax.shard_map(
        per_device,
        mesh=grid,
        in_specs=placed,
        out_specs=(P("grp", slab, None), P("grp")),
        check_vma=False,
    )
```

```python
import numpy as np

import jax
import jax.numpy as jnp
from jax import lax
from jax.experimental import pallas as pl
from jax.experimental.pallas import tpu as pltpu
from jax.sharding import Mesh, PartitionSpec as P
import ml_dtypes

BAND = 128
HALF = BAND // 2
WIN = 128
TILTS = 2
INNER = 16
PAIRS = HALF // INNER
ROWS = 136
LANES = 128
CH_IN = 12 * PAIRS
CH_MID = 16 * PAIRS
CH_OUT = 24


def split(table):
    table = np.asarray(table, np.float32)
    high = table.astype(ml_dtypes.bfloat16)
    low = (table - high.astype(np.float32)).astype(ml_dtypes.bfloat16)
    return high, low


def turns(a, b, length):
    angle = (a[:, None].astype(np.int64) * b[None, :]) % length * (2.0 * np.pi / length)
    return np.cos(angle), np.sin(angle)


def row_table(length):
    c, s = turns(np.arange(HALF + 1), np.arange(length), length)
    out = np.zeros((ROWS, length))
    out[:HALF] = c[:HALF]
    out[HALF] = c[HALF]
    out[HALF + 1 : BAND] = s[1:HALF]
    out[BAND] = s[HALF]
    high, low = split(out)
    return np.concatenate([high, low])


def column_table(length):
    c, s = turns(np.arange(length), np.arange(BAND), length)
    high, low = split(np.concatenate([c, s], 1))
    return np.stack([high, low])


def window_column_table(length):
    c, s = turns(np.arange(BAND), np.arange(WIN) - WIN // 2, length)
    high, low = split(np.concatenate([c, -s], 0))
    return np.stack([high, low])


def window_row_table(length):
    c, s = turns(np.arange(WIN) - WIN // 2, np.arange(HALF + 1), length)
    out = np.zeros((TILTS, WIN, INNER, CH_OUT))
    for t in range(TILTS):
        for k in range(INNER):
            for r in range(PAIRS):
                p = k * PAIRS + r
                out[t, :, k, 2 * PAIRS * t + r] = c[:, p]
                out[t, :, k, 2 * PAIRS * t + PAIRS + r] = -s[:, p] if p else c[:, HALF]
        out[t, :, 0, 4 * PAIRS + t] = s[:, HALF]
    high, low = split(out.reshape(TILTS * WIN, INNER * CH_OUT))
    return np.stack([high, low])


def dot(a, b):
    return jnp.dot(a, b, preferred_element_type=jnp.float32)


def halves(x):
    high = x.astype(jnp.bfloat16)
    return high, (x - high.astype(jnp.float32)).astype(jnp.bfloat16)


def spectrum_kernel(
    h_shift, h_weight, h_center, h_owner, h_volume, h_row, h_col, h_left, h_share, h_ref, out, aux,
    shift, weight, center, owner, volume, row_tab, col_tab, left, share, ref,
    rpad, sums, lhs, proj, band, sem, vsem,
):
    planes, height, width = h_volume.shape
    tiles = width // LANES
    step = 256
    steps = width // step

    def fetch(src, dst, i):
        copy = pltpu.make_async_copy(src, dst, sem.at[i])
        copy.start()
        return copy

    get_row = fetch(h_row, row_tab, 0)
    blocks = []
    for z in range(planes):
        for n in range(steps):
            i = z * steps + n
            cols = pl.ds(n * step, step)
            copy = pltpu.make_async_copy(h_volume.at[z, :, cols], volume.at[i], vsem.at[i])
            copy.start()
            blocks.append(copy)
            if i == 0:
                get_center = fetch(h_center, center, 1)
                get_owner = fetch(h_owner, owner, 2)
                get_shift = fetch(h_shift, shift, 3)
                get_weight = fetch(h_weight, weight, 4)
    get_left = fetch(h_left, left, 5)
    get_share = fetch(h_share, share, 6)
    get_ref = fetch(h_ref, ref, 7)
    get_col = fetch(h_col, col_tab, 8)

    line = lax.axis_index("line")
    seat = lax.axis_index("seat")
    rpad[:, :, :LANES] = jnp.zeros((planes, ROWS, LANES), jnp.float32)
    rpad[:, :, LANES + width :] = jnp.zeros((planes, ROWS, LANES), jnp.float32)
    get_center.wait()
    get_owner.wait()
    row = lax.broadcasted_iota(jnp.int32, (2 * PAIRS, BAND), 0)
    b = lax.broadcasted_iota(jnp.int32, (2 * PAIRS, BAND), 1)
    p = seat * PAIRS + (row & (PAIRS - 1))
    q = jnp.where(row < PAIRS, p, jnp.where(p == 0, -HALF, -p))
    who = lax.broadcasted_iota(jnp.int32, (INNER, BAND), 0) + line * INNER
    for t in range(TILTS):
        turn = (q * center[t, 0] + b * center[t, 1]) & (width - 1)
        angle = turn.astype(jnp.float32) * (2.0 * np.pi / width)
        at = t * (4 * PAIRS + INNER)
        aux[at : at + 2 * PAIRS, :] = jnp.cos(angle)
        aux[at + 2 * PAIRS : at + 4 * PAIRS, :] = jnp.sin(angle)
        aux[at + 4 * PAIRS : at + 4 * PAIRS + INNER, :] = jnp.where(who == owner[t], 1.0, 0.0)

    get_row.wait()
    for z in range(planes):
        for n in range(steps):
            i = z * steps + n
            blocks[i].wait()
            r = dot(row_tab[...], volume[i])
            at = LANES + n * step
            rpad[z, :, at : at + step] = r[:ROWS] + r[ROWS:]
    get_shift.wait()
    get_weight.wait()
    get_left.wait()
    get_share.wait()
    lane = lax.broadcasted_iota(jnp.int32, (8, LANES), 1)
    for t in range(TILTS):
        moves = []
        for z in range(planes):
            w = weight[t, z]
            for more, factor in ((0, 1.0 - w), (1, w)):
                s = shift[t, z] + more
                turn = jnp.where(s < 0, s + LANES, s)
                moves.append((z, jnp.where(s < 0, 1, 0), turn, lane < turn, factor))
        for g in range(ROWS // 8):
            rows = slice(g * 8, g * 8 + 8)
            total = [None] * tiles
            for z, off, turn, mask, factor in moves:
                turned = []
                for j in range(tiles + 1):
                    at = pl.multiple_of((j + off) * LANES, LANES)
                    turned.append(pltpu.roll(rpad[z, rows, pl.ds(at, LANES)], turn, 1))
                for j in range(tiles):
                    term = factor * jnp.where(mask, turned[j], turned[j + 1])
                    total[j] = term if total[j] is None else total[j] + term
            for j in range(tiles):
                sums[rows, j * LANES : (j + 1) * LANES] = total[j]
        here = sums[:ROWS, :]
        sums[ROWS:, :] = pltpu.roll(here, width - 1, 1)
        high, low = halves(sums[...])
        lhs[: 2 * ROWS] = high
        lhs[2 * ROWS :] = low
        place = lax.broadcasted_iota(jnp.int32, (width, step), 0)
        for n in range(0, width, step):
            pick = jnp.where(place == left[t : t + 1, n : n + step], 1.0, 0.0).astype(jnp.bfloat16)
            y = dot(lhs[...], pick)
            y = y[: 2 * ROWS] + y[2 * ROWS :]
            cw = share[t : t + 1, n : n + step]
            proj[t * ROWS : (t + 1) * ROWS, n : n + step] = (1.0 - cw) * y[:ROWS] + cw * y[ROWS:]
    get_col.wait()
    high, low = halves(proj[...])
    band[...] = dot(high, col_tab[0]) + dot(low, col_tab[0]) + dot(high, col_tab[1])
    for t in range(TILTS):
        b = t * ROWS
        row = band[b + HALF : b + HALF + 1, :]
        last = band[b + BAND : b + BAND + 1, :]
        band[b + HALF : b + HALF + 1, :BAND] = row[:, :BAND] + last[:, BAND:]
        band[b + HALF : b + HALF + 1, BAND:] = row[:, BAND:] - last[:, :BAND]
    get_ref.wait()
    for k in range(INNER):
        for t in range(TILTS):
            for i, (r0, c0) in enumerate(((0, 0), (0, BAND), (HALF, 0), (HALF, BAND))):
                at = t * ROWS + r0 + k * PAIRS
                to = (4 * t + i) * PAIRS
                out[k, to : to + PAIRS, :] = band[at : at + PAIRS, c0 : c0 + BAND]
        for i in range(2):
            to = (8 + i) * PAIRS
            a = HALF + k * PAIRS
            out[k, to : to + PAIRS, :] = ref[0, i, a : a + PAIRS, :]
            for r in range(PAIRS):
                p = k * PAIRS + r
                a = HALF - p if p else 0
                to = (10 + i) * PAIRS + r
                out[k, to : to + 1, :] = ref[0, i, a : a + 1, :]


def row_sum_kernel(aux, got, out):
    n = got.shape[0]
    total = got[0, : 8 * PAIRS, :]
    for s in range(1, n):
        total = total + got[s, : 8 * PAIRS, :]
    refs = []
    for t in range(TILTS):
        at = t * (4 * PAIRS + INNER) + 4 * PAIRS
        chosen = jnp.zeros((4 * PAIRS, BAND), jnp.float32)
        for s in range(n):
            chosen = jnp.where(aux[at + s : at + s + 1, :] > 0.5, got[s, 8 * PAIRS :, :], chosen)
        refs.append(chosen)
    for y in range(out.shape[0]):
        out[y, : 8 * PAIRS, :] = total
        for t in range(TILTS):
            out[y, (8 + 4 * t) * PAIRS : (12 + 4 * t) * PAIRS, :] = refs[t]


def cross_kernel(aux, got, tab, out, lhs):
    n = got.shape[0]
    total = got[0]
    for s in range(1, n):
        total = total + got[s]
    zero = lax.axis_index("seat") * PAIRS + lax.broadcasted_iota(jnp.int32, (PAIRS, BAND), 0) == 0
    lhs[...] = jnp.zeros(lhs.shape, jnp.float32)
    energies = []
    for t in range(TILTS):

        def part(i):
            return total[i * PAIRS : (i + 1) * PAIRS, :]

        cc, cs, sc, ss = (part(4 * t + i) for i in range(4))
        refs = [part(8 + 4 * t + i) for i in range(4)]
        plus = (jnp.where(zero, cc, cc - ss), -jnp.where(zero, cs, cs + sc))
        minus = (jnp.where(zero, sc, cc + ss), -jnp.where(zero, ss, cs - sc))
        crossed = []
        e_spec = e_ref = 0.0
        for i, ((sr, si), (rr, ri)) in enumerate(((plus, refs[:2]), (minus, refs[2:]))):
            cr = sr * rr + si * ri
            ci = si * rr - sr * ri
            e_spec = e_spec + sr * sr + si * si
            e_ref = e_ref + rr * rr + ri * ri
            at = t * (4 * PAIRS + INNER) + i * PAIRS
            co = aux[at : at + PAIRS, :]
            sn = aux[at + 2 * PAIRS : at + 3 * PAIRS, :]
            crossed.append((cr * co - ci * sn, cr * sn + ci * co))
        (pr, pi), (mr, mi) = crossed
        at = 2 * PAIRS * t
        lhs[at : at + PAIRS, :BAND] = jnp.where(zero, pr, pr + mr)
        lhs[at : at + PAIRS, BAND:] = jnp.where(zero, pi, pi + mi)
        lhs[at + PAIRS : at + 2 * PAIRS, :BAND] = jnp.where(zero, mr, pi - mi)
        lhs[at + PAIRS : at + 2 * PAIRS, BAND:] = jnp.where(zero, mi, mr - pr)
        extra = 4 * PAIRS + t
        lhs[extra : extra + 1, :BAND] = mi[:1]
        lhs[extra : extra + 1, BAND:] = -mr[:1]
        energies += [jnp.sum(e_spec, 0, keepdims=True), jnp.sum(e_ref, 0, keepdims=True)]
    high, low = halves(lhs[...])
    h = dot(high, tab[0]) + dot(low, tab[0]) + dot(high, tab[1])
    h = h[:CH_OUT]
    for d in range(out.shape[0]):
        out[d] = h
        for i, e in enumerate(energies):
            to = 4 * PAIRS + TILTS + i
            out[d, to : to + 1, :] = e


def window_kernel(got, tab, rows, peaks, corr):
    x = got[...].reshape(got.shape[0] * CH_OUT, WIN)
    high, low = halves(x)
    c = dot(tab[0], high) + dot(tab[0], low) + dot(tab[1], high)
    e = jnp.sum(jnp.sum(got[:, 4 * PAIRS + TILTS :, :], 0), 1, keepdims=True)
    mine_row = lax.axis_index("line") * INNER + lax.axis_index("seat")
    for t in range(TILTS):
        spec = e[2 * t : 2 * t + 1] / (BAND * BAND) + 1e-06
        ref = e[2 * t + 1 : 2 * t + 2] / (BAND * BAND) + 1e-06
        mine = c[t * WIN : (t + 1) * WIN] / (BAND * jnp.sqrt(spec * ref))
        corr[t] = mine
        peaks[t] = jnp.max(mine)
        rows[t] = corr[t, pl.ds(mine_row, 1), :]


def solution(mesh):
    outer = mesh.shape["slab"] // INNER
    grid = Mesh(
        mesh.devices.reshape(mesh.shape["grp"], outer, INNER), ("grp", "line", "seat")
    )
    slab = ("line", "seat")
    vmem = pl.BlockSpec(memory_space=pltpu.VMEM)
    smem = pl.BlockSpec(memory_space=pltpu.SMEM)
    hbm = pl.BlockSpec(memory_space=pltpu.HBM)
    small = pltpu.CompilerParams(vmem_limit_bytes=4 * 1024 * 1024)
    f32, bf16 = jnp.float32, jnp.bfloat16

    def per_device(volume, shift, weight, left, share, center, owner, ref):
        planes, height, width = volume.shape
        row_tab = jnp.asarray(row_table(height))
        col_tab = jnp.asarray(column_table(width))
        blocks = planes * width // 256
        packed, aux = pl.pallas_call(
            spectrum_kernel,
            out_shape=[
                jax.ShapeDtypeStruct((INNER, CH_IN, BAND), f32),
                jax.ShapeDtypeStruct((TILTS * (4 * PAIRS + INNER), BAND), f32),
            ],
            in_specs=[hbm] * 10,
            out_specs=[vmem] * 2,
            scratch_shapes=[
                pltpu.SMEM(shift.shape, jnp.int32),
                pltpu.SMEM(weight.shape, f32),
                pltpu.SMEM(center.shape, jnp.int32),
                pltpu.SMEM(owner.shape, jnp.int32),
                pltpu.VMEM((blocks, height, 256), bf16),
                pltpu.VMEM(row_tab.shape, bf16),
                pltpu.VMEM(col_tab.shape, bf16),
                pltpu.VMEM(left.shape, jnp.int32),
                pltpu.VMEM(share.shape, f32),
                pltpu.VMEM(ref.shape, f32),
                pltpu.VMEM((planes, ROWS, width + 2 * LANES), f32),
                pltpu.VMEM((2 * ROWS, width), f32),
                pltpu.VMEM((4 * ROWS, width), bf16),
                pltpu.VMEM((TILTS * ROWS, width), f32),
                pltpu.VMEM((TILTS * ROWS, 2 * BAND), f32),
                pltpu.SemaphoreType.DMA((9,)),
                pltpu.SemaphoreType.DMA((blocks,)),
            ],
            compiler_params=pltpu.CompilerParams(vmem_limit_bytes=32 * 1024 * 1024),
            name="spectrum",
        )(*(pltpu.with_memory_space_constraint(a, pltpu.HBM) for a in (shift, weight, center, owner, volume, row_tab, col_tab, left, share, ref)))
        got = lax.all_to_all(packed, "seat", 0, 0, tiled=True)
        summed = pl.pallas_call(
            row_sum_kernel,
            out_shape=jax.ShapeDtypeStruct((outer, CH_MID, BAND), f32),
            in_specs=[vmem] * 2,
            out_specs=vmem,
            compiler_params=small,
            name="row_sum",
        )(aux, got)
        got = lax.all_to_all(summed, "line", 0, 0, tiled=True)
        piece = pl.pallas_call(
            cross_kernel,
            out_shape=jax.ShapeDtypeStruct((INNER, CH_OUT, WIN), f32),
            in_specs=[vmem] * 3,
            out_specs=vmem,
            scratch_shapes=[pltpu.VMEM((32, 2 * BAND), f32)],
            compiler_params=small,
            name="cross",
        )(aux, got, jnp.asarray(window_column_table(width)))
        got = lax.all_to_all(piece, "seat", 0, 0, tiled=True)
        rows, peaks = pl.pallas_call(
            window_kernel,
            out_shape=[jax.ShapeDtypeStruct((TILTS, 1, WIN), f32), jax.ShapeDtypeStruct((TILTS,), f32)],
            in_specs=[vmem] * 2,
            out_specs=[vmem, smem],
            scratch_shapes=[pltpu.VMEM((TILTS, WIN, WIN), f32)],
            compiler_params=small,
            name="window",
        )(got, jnp.asarray(window_row_table(height)))
        return rows, peaks

    placed = (
        P(("grp",) + slab, None, None),
        P("grp", slab),
        P("grp", slab),
        P("grp", None),
        P("grp", None),
        P("grp", None),
        P("grp"),
        P(("grp",) + slab, None, None, None),
    )
    return jax.shard_map(
        per_device,
        mesh=grid,
        in_specs=placed,
        out_specs=(P("grp", slab, None), P("grp")),
        check_vma=False,
    )
```

```python
import numpy as np

import jax
import jax.numpy as jnp
from jax import lax
from jax.experimental import pallas as pl
from jax.experimental.pallas import tpu as pltpu
from jax.sharding import Mesh, PartitionSpec as P
import ml_dtypes

BAND = 128
HALF = BAND // 2
WIN = 128
TILTS = 2
CORES = 2
COLS = 8
ROWS = 136
LANES = 128
CHUNK = 8
CH_OUT = 4


def split(table):
    table = np.asarray(table, np.float32)
    high = table.astype(ml_dtypes.bfloat16)
    low = (table - high.astype(np.float32)).astype(ml_dtypes.bfloat16)
    return high, low


def turns(a, b, length):
    angle = (a[:, None].astype(np.int64) * b[None, :]) % length * (2.0 * np.pi / length)
    return np.cos(angle), np.sin(angle)


def row_table(length):
    c, s = turns(np.arange(HALF + 1), np.arange(length), length)
    out = np.zeros((ROWS, length))
    out[:HALF] = c[:HALF]
    out[HALF] = c[HALF]
    out[HALF + 1 : BAND] = s[1:HALF]
    out[BAND] = s[HALF]
    high, low = split(out)
    return np.concatenate([high, low])


def column_table(length):
    c, s = turns(np.arange(length), np.arange(BAND), length)
    high, low = split(np.concatenate([c, s], 1))
    return np.stack([high, low])


def window_column_table(length):
    c, s = turns(np.arange(BAND), np.arange(WIN) - WIN // 2, length)
    high, low = split(np.concatenate([c, -s], 0))
    return np.stack([high, low])


def window_row_table(length):
    c, s = turns(np.arange(WIN) - WIN // 2, np.arange(HALF + 1), length)
    out = np.zeros((WIN, HALF, CH_OUT))
    out[:, :, 0] = c[:, :HALF]
    out[:, 1:, 1] = -s[:, 1:HALF]
    out[:, 0, 1] = c[:, HALF]
    out[:, 0, 2] = s[:, HALF]
    high, low = split(out.reshape(WIN, HALF * CH_OUT))
    return np.stack([high, low])


def dot(a, b):
    return jnp.dot(a, b, preferred_element_type=jnp.float32)


def halves(x):
    high = x.astype(jnp.bfloat16)
    return high, (x - high.astype(jnp.float32)).astype(jnp.bfloat16)


def shift_kernel(
    h_shift, h_weight, h_center, h_owner, h_volume, h_row, h_ref, keep, send, aux,
    shift, weight, center, owner, volume, row_tab, rpad, sem, vsem,
):
    planes, height, width = h_volume.shape
    tiles = width // LANES
    step = 256
    steps = height // step

    def fetch(src, dst, i):
        copy = pltpu.make_async_copy(src, dst, sem.at[i])
        copy.start()
        return copy

    get_row = fetch(h_row, row_tab, 0)
    blocks = []
    for z in range(planes):
        for n in range(steps):
            i = z * steps + n
            cut = pl.ds(n * step, step)
            copy = pltpu.make_async_copy(h_volume.at[z, cut, :], volume.at[z, cut, :], vsem.at[i])
            copy.start()
            blocks.append(copy)
            if i == 0:
                get_center = fetch(h_center, center, 1)
                get_owner = fetch(h_owner, owner, 2)
                get_shift = fetch(h_shift, shift, 3)
                get_weight = fetch(h_weight, weight, 4)
    refs = [fetch(h_ref.at[0, i], send.at[pl.ds(tiles * ROWS + i * BAND, BAND), :], 5 + i) for i in range(2)]

    col = lax.axis_index("col")
    core = lax.axis_index("core")
    rpad[:, :, :LANES] = jnp.zeros((planes, ROWS, LANES), jnp.float32)
    rpad[:, :, LANES + width :] = jnp.zeros((planes, ROWS, LANES), jnp.float32)
    get_center.wait()
    get_owner.wait()
    pair = lax.axis_index("line") * COLS + col
    row = lax.broadcasted_iota(jnp.int32, (8, BAND), 0)
    b = lax.broadcasted_iota(jnp.int32, (8, BAND), 1)
    q = jnp.where(row == 0, pair, jnp.where(pair == 0, -HALF, -pair))
    turn = (q * center[core, 0] + b * center[core, 1]) & (width - 1)
    angle = turn.astype(jnp.float32) * (2.0 * np.pi / width)
    aux[:8, :] = jnp.cos(angle)
    aux[8:16, :] = jnp.sin(angle)
    who = pair * CORES + jnp.where(row == 0, core, 1 - core)
    aux[16:, :] = jnp.where(who == owner[core], 1.0, 0.0)

    get_row.wait()
    for z in range(planes):
        for n in range(steps):
            blocks[z * steps + n].wait()
        for n in range(0, width, step):
            r = dot(row_tab[...], volume[z, :, n : n + step])
            rpad[z, :, LANES + n : LANES + n + step] = r[:ROWS] + r[ROWS:]
    get_shift.wait()
    get_weight.wait()
    lane = lax.broadcasted_iota(jnp.int32, (8, LANES), 1)
    for t, out in ((1 - core, send), (core, keep)):
        moves = []
        for z in range(planes):
            w = weight[t, z]
            for more, factor in ((0, 1.0 - w), (1, w)):
                s = shift[t, z] + more
                turn = jnp.where(s < 0, s + LANES, s)
                moves.append((z, jnp.where(s < 0, 1, 0), turn, lane < turn, factor))
        for g in range(ROWS // 8):
            rows = slice(g * 8, g * 8 + 8)
            total = [None] * tiles
            for z, off, turn, mask, factor in moves:
                turned = []
                for j in range(tiles + 1):
                    at = pl.multiple_of((j + off) * LANES, LANES)
                    turned.append(pltpu.roll(rpad[z, rows, pl.ds(at, LANES)], turn, 1))
                for j in range(tiles):
                    term = factor * jnp.where(mask, turned[j], turned[j + 1])
                    total[j] = term if total[j] is None else total[j] + term
            for j in range(tiles):
                at = j * ROWS + g * 8
                out[at : at + 8, :] = total[j]
    for copy in refs:
        copy.wait()


def band_kernel(keep, sent, came, aux, left, share, col_tab, out, sums, lhs, proj, band, own):
    width = left.shape[1]
    tiles = width // LANES
    step = 256
    core = lax.axis_index("core")
    for j in range(tiles):
        rows = slice(j * ROWS, (j + 1) * ROWS)
        sums[:ROWS, j * LANES : (j + 1) * LANES] = keep[rows, :] + came[rows, :]
    sums[ROWS:, :] = pltpu.roll(sums[:ROWS, :], width - 1, 1)
    high, low = halves(sums[...])
    lhs[: 2 * ROWS] = high
    lhs[2 * ROWS :] = low
    place = lax.broadcasted_iota(jnp.int32, (width, step), 0)
    for n in range(0, width, step):
        pick = jnp.where(place == left[pl.ds(core, 1), n : n + step], 1.0, 0.0).astype(jnp.bfloat16)
        y = dot(lhs[...], pick)
        y = y[: 2 * ROWS] + y[2 * ROWS :]
        cw = share[pl.ds(core, 1), n : n + step]
        proj[:, n : n + step] = (1.0 - cw) * y[:ROWS] + cw * y[ROWS:]
    high, low = halves(proj[...])
    band[...] = dot(high, col_tab[0]) + dot(low, col_tab[0]) + dot(high, col_tab[1])
    row = band[HALF : HALF + 1, :]
    last = band[BAND : BAND + 1, :]
    band[HALF : HALF + 1, :BAND] = row[:, :BAND] + last[:, BAND:]
    band[HALF : HALF + 1, BAND:] = row[:, BAND:] - last[:, :BAND]
    mine = aux[16:17, :] > 0.5
    theirs = aux[17:18, :] > 0.5
    for i in range(2):
        at = slice(tiles * ROWS + i * BAND, tiles * ROWS + (i + 1) * BAND)
        own[i] = jnp.where(mine, sent[at, :], jnp.where(theirs, came[at, :], 0.0))
    for p in range(HALF):
        minus = HALF - p if p else 0
        for i in range(2):
            out[p, i : i + 1, :] = band[p : p + 1, i * BAND : (i + 1) * BAND]
            out[p, 2 + i : 3 + i, :] = band[HALF + p : HALF + p + 1, i * BAND : (i + 1) * BAND]
            out[p, 4 + i : 5 + i, :] = own[i, HALF + p : HALF + p + 1, :]
            out[p, 6 + i : 7 + i, :] = own[i, minus : minus + 1, :]


def cross_kernel(aux, got, tab, out, lhs):
    n = got.shape[0]
    parts = [got[i] for i in range(8)]
    for i in range(8, n):
        parts[i % 8] = parts[i % 8] + got[i]
    while len(parts) > 1:
        parts = [parts[i] + parts[i + 1] for i in range(0, len(parts), 2)]
    total = parts[0]
    pair = lax.axis_index("line") * COLS + lax.axis_index("col")
    zero = lax.broadcasted_iota(jnp.int32, (1, BAND), 1) * 0 + pair == 0
    cc, cs, sc, ss, *refs = (total[i : i + 1, :] for i in range(8))
    plus = (jnp.where(zero, cc, cc - ss), -jnp.where(zero, cs, cs + sc))
    minus = (jnp.where(zero, sc, cc + ss), -jnp.where(zero, ss, cs - sc))
    crossed = []
    e_spec = e_ref = 0.0
    for i, ((sr, si), (rr, ri)) in enumerate(((plus, refs[:2]), (minus, refs[2:]))):
        cr = sr * rr + si * ri
        ci = si * rr - sr * ri
        e_spec = e_spec + sr * sr + si * si
        e_ref = e_ref + rr * rr + ri * ri
        co = aux[i : i + 1, :]
        sn = aux[8 + i : 9 + i, :]
        crossed.append((cr * co - ci * sn, cr * sn + ci * co))
    (pr, pi), (mr, mi) = crossed
    lhs[...] = jnp.zeros(lhs.shape, jnp.float32)
    lhs[0:1, :BAND] = jnp.where(zero, pr, pr + mr)
    lhs[0:1, BAND:] = jnp.where(zero, pi, pi + mi)
    lhs[1:2, :BAND] = jnp.where(zero, mr, pi - mi)
    lhs[1:2, BAND:] = jnp.where(zero, mi, mr - pr)
    lhs[2:3, :BAND] = mi
    lhs[2:3, BAND:] = -mr
    high, low = halves(lhs[...])
    h = dot(high, tab[0]) + dot(low, tab[0]) + dot(high, tab[1])
    lane = lax.broadcasted_iota(jnp.int32, (1, BAND), 1)
    e_spec = jnp.sum(e_spec, 1, keepdims=True)
    e_ref = jnp.sum(e_ref, 1, keepdims=True)
    lhs[:8, :BAND] = h[:8]
    lhs[3:4, :BAND] = jnp.where(lane < BAND // 2, e_spec, e_ref)
    done = lhs[:CH_OUT, :BAND]
    for d in range(out.shape[0]):
        out[d] = done


def window_kernel(got, tab, send, keep):
    n = got.shape[0]
    mine_row = (lax.axis_index("line") * COLS + lax.axis_index("col")) * CORES + lax.axis_index("core")
    high, low = halves(got[...].reshape(n * CH_OUT, WIN))
    c = dot(tab[0], high) + dot(tab[0], low) + dot(tab[1], high)
    e = jnp.sum(got[:, CH_OUT - 1, :], 0, keepdims=True)
    spec = e[:, :1] / (BAND * BAND) + 1e-06
    ref = e[:, BAND - 1 :] / (BAND * BAND) + 1e-06
    c = c / (BAND * jnp.sqrt(spec * ref))
    peak = jnp.max(c)
    index = lax.broadcasted_iota(jnp.int32, (WIN, WIN), 0)
    for out, row in ((keep, mine_row), (send, mine_row ^ 1)):
        out[0:1, :] = jnp.sum(jnp.where(index == row, c, 0.0), 0, keepdims=True)
        out[1:2, :] = jnp.full((1, WIN), peak)


def join_kernel(keep, came, rows, peaks):
    core = lax.axis_index("core")
    rows[pl.ds(core, 1), 0, :] = keep[0:1, :]
    rows[pl.ds(1 - core, 1), 0, :] = came[0:1, :]
    peaks[core] = jnp.max(keep[1:2, :])
    peaks[1 - core] = jnp.max(came[1:2, :])


def solution(mesh):
    lines = mesh.shape["slab"] // (COLS * CORES)
    grid = Mesh(
        mesh.devices.reshape(mesh.shape["grp"], lines, COLS, CORES), ("grp", "line", "col", "core")
    )
    slab = ("line", "col", "core")
    vmem = pl.BlockSpec(memory_space=pltpu.VMEM)
    smem = pl.BlockSpec(memory_space=pltpu.SMEM)
    hbm = pl.BlockSpec(memory_space=pltpu.HBM)
    small = pltpu.CompilerParams(vmem_limit_bytes=4 * 1024 * 1024)
    f32, bf16 = jnp.float32, jnp.bfloat16

    def per_device(volume, shift, weight, left, share, center, owner, ref):
        planes, height, width = volume.shape
        row_tab = jnp.asarray(row_table(height))
        col_tab = jnp.asarray(column_table(width))
        tiles = width // LANES
        blocks = planes * height // 256
        fetched = (shift, weight, center, owner, volume, row_tab, ref)
        keep, send, aux = pl.pallas_call(
            shift_kernel,
            out_shape=[
                jax.ShapeDtypeStruct((tiles * ROWS, LANES), f32),
                jax.ShapeDtypeStruct((tiles * ROWS + 2 * BAND, LANES), f32),
                jax.ShapeDtypeStruct((24, BAND), f32),
            ],
            in_specs=[hbm] * len(fetched),
            out_specs=[vmem] * 3,
            scratch_shapes=[
                pltpu.SMEM(shift.shape, jnp.int32),
                pltpu.SMEM(weight.shape, f32),
                pltpu.SMEM(center.shape, jnp.int32),
                pltpu.SMEM(owner.shape, jnp.int32),
                pltpu.VMEM(volume.shape, bf16),
                pltpu.VMEM(row_tab.shape, bf16),
                pltpu.VMEM((planes, ROWS, width + 2 * LANES), f32),
                pltpu.SemaphoreType.DMA((7,)),
                pltpu.SemaphoreType.DMA((blocks,)),
            ],
            compiler_params=pltpu.CompilerParams(vmem_limit_bytes=24 * 1024 * 1024),
            name="shift",
        )(*(pltpu.with_memory_space_constraint(a, pltpu.HBM) for a in fetched))
        came = lax.ppermute(send, "core", [(i, (i + 1) % CORES) for i in range(CORES)])
        packed = pl.pallas_call(
            band_kernel,
            out_shape=jax.ShapeDtypeStruct((HALF, CHUNK, BAND), f32),
            in_specs=[vmem] * 7,
            out_specs=vmem,
            scratch_shapes=[
                pltpu.VMEM((2 * ROWS, width), f32),
                pltpu.VMEM((4 * ROWS, width), bf16),
                pltpu.VMEM((ROWS, width), f32),
                pltpu.VMEM((ROWS, 2 * BAND), f32),
                pltpu.VMEM((2, BAND, BAND), f32),
            ],
            compiler_params=pltpu.CompilerParams(vmem_limit_bytes=24 * 1024 * 1024),
            name="band",
        )(keep, send, came, aux, left, share, col_tab)
        got = lax.all_to_all(packed, ("line", "col"), 0, 0, tiled=True)
        piece = pl.pallas_call(
            cross_kernel,
            out_shape=jax.ShapeDtypeStruct((HALF, CH_OUT, WIN), f32),
            in_specs=[vmem] * 3,
            out_specs=vmem,
            scratch_shapes=[pltpu.VMEM((16, 2 * BAND), f32)],
            compiler_params=small,
            name="cross",
        )(aux, got, jnp.asarray(window_column_table(width)))
        got = lax.all_to_all(piece, ("line", "col"), 0, 0, tiled=True)
        send, keep = pl.pallas_call(
            window_kernel,
            out_shape=[jax.ShapeDtypeStruct((2, WIN), f32)] * 2,
            in_specs=[vmem] * 2,
            out_specs=[vmem] * 2,
            compiler_params=small,
            name="window",
        )(got, jnp.asarray(window_row_table(height)))
        came = lax.ppermute(send, "core", [(i, (i + 1) % CORES) for i in range(CORES)])
        return pl.pallas_call(
            join_kernel,
            out_shape=[jax.ShapeDtypeStruct((TILTS, 1, WIN), f32), jax.ShapeDtypeStruct((TILTS,), f32)],
            in_specs=[vmem] * 2,
            out_specs=[vmem, smem],
            compiler_params=small,
            name="join",
        )(keep, came)

    placed = (
        P(("grp",) + slab, None, None),
        P("grp", slab),
        P("grp", slab),
        P("grp", None),
        P("grp", None),
        P("grp", None),
        P("grp"),
        P(("grp",) + slab, None, None, None),
    )
    return jax.shard_map(
        per_device,
        mesh=grid,
        in_specs=placed,
        out_specs=(P("grp", slab, None), P("grp")),
        check_vma=False,
    )
```

```python
import numpy as np

import jax
import jax.numpy as jnp
from jax import lax
from jax.experimental import pallas as pl
from jax.experimental.pallas import tpu as pltpu
from jax.sharding import Mesh, PartitionSpec as P
import ml_dtypes

BAND = 128
HALF = BAND // 2
WIN = 128
TILTS = 2
CORES = 2
COLS = 8
ROWS = 136
LANES = 128
VPARTS = 2
CHUNK = 8
CH_OUT = 4


def split(table):
    table = np.asarray(table, np.float32)
    high = table.astype(ml_dtypes.bfloat16)
    low = (table - high.astype(np.float32)).astype(ml_dtypes.bfloat16)
    return high, low


def turns(a, b, length):
    angle = (a[:, None].astype(np.int64) * b[None, :]) % length * (2.0 * np.pi / length)
    return np.cos(angle), np.sin(angle)


def row_table(length):
    c, s = turns(np.arange(HALF + 1), np.arange(length), length)
    out = np.zeros((ROWS, length))
    out[:HALF] = c[:HALF]
    out[HALF] = c[HALF]
    out[HALF + 1 : BAND] = s[1:HALF]
    out[BAND] = s[HALF]
    high, low = split(out)
    return np.concatenate([high, low])


def column_table(length):
    c, s = turns(np.arange(length), np.arange(BAND), length)
    high, low = split(np.concatenate([c, s], 1))
    return np.stack([high, low])


def window_column_table(length):
    c, s = turns(np.arange(BAND), np.arange(WIN) - WIN // 2, length)
    high, low = split(np.concatenate([c, -s], 0))
    return np.stack([high, low])


def window_row_table(length):
    c, s = turns(np.arange(WIN) - WIN // 2, np.arange(HALF + 1), length)
    out = np.zeros((WIN, HALF, CH_OUT))
    out[:, :, 0] = c[:, :HALF]
    out[:, 1:, 1] = -s[:, 1:HALF]
    out[:, 0, 1] = c[:, HALF]
    out[:, 0, 2] = s[:, HALF]
    high, low = split(out.reshape(WIN, HALF * CH_OUT))
    return np.stack([high, low])


def dot(a, b):
    return jnp.dot(a, b, preferred_element_type=jnp.float32)


def halves(x):
    high = x.astype(jnp.bfloat16)
    return high, (x - high.astype(jnp.float32)).astype(jnp.bfloat16)


def shift_kernel(
    h_shift, h_weight, h_center, h_owner, h_volume, h_row, h_ref, keep, send, aux,
    shift, weight, center, owner, volume, row_tab, *rest,
):
    planes, height, width = h_volume.shape
    rpads, sem, vsem = rest[: 2 * planes], rest[-2], rest[-1]
    tiles = width // LANES
    step = 256
    part = width // VPARTS

    def fetch(src, dst, i):
        copy = pltpu.make_async_copy(src, dst, sem.at[i])
        copy.start()
        return copy

    get_row = fetch(h_row, row_tab, 0)
    blocks = []
    for z in range(planes):
        for n in range(VPARTS):
            i = z * VPARTS + n
            cut = pl.ds(n * part, part)
            copy = pltpu.make_async_copy(h_volume.at[z, :, cut], volume.at[i], vsem.at[i])
            copy.start()
            blocks.append(copy)
            if i == 0:
                get_center = fetch(h_center, center, 1)
                get_owner = fetch(h_owner, owner, 2)
                get_shift = fetch(h_shift, shift, 3)
                get_weight = fetch(h_weight, weight, 4)
    refs = [fetch(h_ref.at[0, i], send.at[pl.ds(tiles * ROWS + i * BAND, BAND), :], 5 + i) for i in range(2)]

    col = lax.axis_index("col")
    core = lax.axis_index("core")
    for pad in rpads:
        pad[:, :LANES] = jnp.zeros((ROWS, LANES), jnp.float32)
        pad[:, LANES + width :] = jnp.zeros((ROWS, LANES), jnp.float32)
    get_center.wait()
    get_owner.wait()
    pair = lax.axis_index("line") * COLS + col
    row = lax.broadcasted_iota(jnp.int32, (8, BAND), 0)
    b = lax.broadcasted_iota(jnp.int32, (8, BAND), 1)
    q = jnp.where(row == 0, pair, jnp.where(pair == 0, -HALF, -pair))
    turn = (q * center[core, 0] + b * center[core, 1]) & (width - 1)
    angle = turn.astype(jnp.float32) * (2.0 * np.pi / width)
    aux[:8, :] = jnp.cos(angle)
    aux[8:16, :] = jnp.sin(angle)
    who = pair * CORES + jnp.where(row == 0, core, 1 - core)
    aux[16:, :] = jnp.where(who == owner[core], 1.0, 0.0)
    get_shift.wait()
    get_weight.wait()
    get_row.wait()

    lane = lax.broadcasted_iota(jnp.int32, (8, LANES), 1)
    first = lane == 0

    def transform(z):
        near = rpads[2 * z]
        for n in range(0, width, step):
            if n % part == 0:
                blocks[z * VPARTS + n // part].wait()
            at = n % part
            r = dot(row_tab[...], volume[z * VPARTS + n // part, :, at : at + step])
            near[:, LANES + n : LANES + n + step] = r[:ROWS] + r[ROWS:]

    def move(z):
        near, far = rpads[2 * z], rpads[2 * z + 1]
        for g in range(ROWS // 8):
            rows = slice(g * 8, g * 8 + 8)
            turned = [pltpu.roll(near[rows, LANES * j : LANES * (j + 1)], 1, 1) for j in range(1, tiles + 1)]
            for j in range(tiles + 1):
                left = turned[j - 1] if j else 0.0
                here = turned[j] if j < tiles else 0.0
                far[rows, LANES * (j + 1) : LANES * (j + 2)] = jnp.where(first, left, here)
        for t, out in ((1 - core, send), (core, keep)):
            w = weight[t, z]
            s = shift[t, z]
            turn = jnp.where(s < 0, s + LANES, s)
            off = jnp.where(s < 0, 1, 0)
            mask = lane < turn
            for g in range(ROWS // 8):
                rows = slice(g * 8, g * 8 + 8)
                turned = []
                for j in range(tiles + 1):
                    at = pl.ds(pl.multiple_of((j + off) * LANES, LANES), LANES)
                    mixed = (1.0 - w) * near[rows, at] + w * far[rows, at]
                    turned.append(pltpu.roll(mixed, turn, 1))
                for j in range(tiles):
                    term = jnp.where(mask, turned[j], turned[j + 1])
                    at = j * ROWS + g * 8
                    out[at : at + 8, :] = term if z == 0 else out[at : at + 8, :] + term

    transform(0)
    for z in range(planes):
        if z + 1 < planes:
            transform(z + 1)
        move(z)
    for copy in refs:
        copy.wait()


def mix_kernel(left, share, col_tab, after, out):
    width = left.shape[1]
    step = 256
    core = lax.axis_index("core")
    at = left[pl.ds(core, 1), :]
    w = share[pl.ds(core, 1), :]
    near_high, near_low = halves(1.0 - w)
    far_high, far_low = halves(w)
    none = jnp.zeros((step, width), jnp.bfloat16)
    x = lax.broadcasted_iota(jnp.int32, (step, width), 0).astype(jnp.float32).astype(jnp.bfloat16)
    for n in range(0, width, step):

        def is_at(place):
            inside = (place >= 0) & (place < step)
            return x == jnp.where(inside, place, -8).astype(jnp.float32).astype(jnp.bfloat16)

        near, far = is_at(at - n), is_at(at + 1 - n)
        high = jnp.where(near, near_high, jnp.where(far, far_high, none))
        low = jnp.where(near, near_low, jnp.where(far, far_low, none))
        y = dot(high, col_tab[0]) + dot(low, col_tab[0]) + dot(high, col_tab[1])
        high, low = halves(y)
        out[0, n : n + step, :] = high
        out[1, n : n + step, :] = low


def band_kernel(keep, sent, came, aux, mixed, out, sums, band, own):
    tiles = keep.shape[0] // ROWS
    for j in range(tiles):
        rows = slice(j * ROWS, (j + 1) * ROWS)
        sums[:, j * LANES : (j + 1) * LANES] = keep[rows, :] + came[rows, :]
    high, low = halves(sums[...])
    band[...] = dot(high, mixed[0]) + dot(low, mixed[0]) + dot(high, mixed[1])
    row = band[HALF : HALF + 1, :]
    last = band[BAND : BAND + 1, :]
    band[HALF : HALF + 1, :BAND] = row[:, :BAND] + last[:, BAND:]
    band[HALF : HALF + 1, BAND:] = row[:, BAND:] - last[:, :BAND]
    mine = aux[16:17, :] > 0.5
    theirs = aux[17:18, :] > 0.5
    for i in range(2):
        at = slice(tiles * ROWS + i * BAND, tiles * ROWS + (i + 1) * BAND)
        own[i] = jnp.where(mine, sent[at, :], jnp.where(theirs, came[at, :], 0.0))
    for p in range(HALF):
        minus = HALF - p if p else 0
        for i in range(2):
            out[p, i : i + 1, :] = band[p : p + 1, i * BAND : (i + 1) * BAND]
            out[p, 2 + i : 3 + i, :] = band[HALF + p : HALF + p + 1, i * BAND : (i + 1) * BAND]
            out[p, 4 + i : 5 + i, :] = own[i, HALF + p : HALF + p + 1, :]
            out[p, 6 + i : 7 + i, :] = own[i, minus : minus + 1, :]


def cross_kernel(aux, got, tab, out, lhs):
    n = got.shape[0]
    parts = [got[i] for i in range(8)]
    for i in range(8, n):
        parts[i % 8] = parts[i % 8] + got[i]
    while len(parts) > 1:
        parts = [parts[i] + parts[i + 1] for i in range(0, len(parts), 2)]
    total = parts[0]
    pair = lax.axis_index("line") * COLS + lax.axis_index("col")
    zero = lax.broadcasted_iota(jnp.int32, (1, BAND), 1) * 0 + pair == 0
    cc, cs, sc, ss, *refs = (total[i : i + 1, :] for i in range(8))
    plus = (jnp.where(zero, cc, cc - ss), -jnp.where(zero, cs, cs + sc))
    minus = (jnp.where(zero, sc, cc + ss), -jnp.where(zero, ss, cs - sc))
    crossed = []
    e_spec = e_ref = 0.0
    for i, ((sr, si), (rr, ri)) in enumerate(((plus, refs[:2]), (minus, refs[2:]))):
        cr = sr * rr + si * ri
        ci = si * rr - sr * ri
        e_spec = e_spec + sr * sr + si * si
        e_ref = e_ref + rr * rr + ri * ri
        co = aux[i : i + 1, :]
        sn = aux[8 + i : 9 + i, :]
        crossed.append((cr * co - ci * sn, cr * sn + ci * co))
    (pr, pi), (mr, mi) = crossed
    lhs[...] = jnp.zeros(lhs.shape, jnp.float32)
    lhs[0:1, :BAND] = jnp.where(zero, pr, pr + mr)
    lhs[0:1, BAND:] = jnp.where(zero, pi, pi + mi)
    lhs[1:2, :BAND] = jnp.where(zero, mr, pi - mi)
    lhs[1:2, BAND:] = jnp.where(zero, mi, mr - pr)
    lhs[2:3, :BAND] = mi
    lhs[2:3, BAND:] = -mr
    high, low = halves(lhs[...])
    h = dot(high, tab[0]) + dot(low, tab[0]) + dot(high, tab[1])
    lane = lax.broadcasted_iota(jnp.int32, (1, BAND), 1)
    e_spec = jnp.sum(e_spec, 1, keepdims=True)
    e_ref = jnp.sum(e_ref, 1, keepdims=True)
    lhs[:8, :BAND] = h[:8]
    lhs[3:4, :BAND] = jnp.where(lane < BAND // 2, e_spec, e_ref)
    done = lhs[:CH_OUT, :BAND]
    for d in range(out.shape[0]):
        out[d] = done


def window_kernel(got, tab, send, keep):
    n = got.shape[0]
    mine_row = (lax.axis_index("line") * COLS + lax.axis_index("col")) * CORES + lax.axis_index("core")
    high, low = halves(got[...].reshape(n * CH_OUT, WIN))
    c = dot(tab[0], high) + dot(tab[0], low) + dot(tab[1], high)
    e = jnp.sum(got[:, CH_OUT - 1, :], 0, keepdims=True)
    spec = e[:, :1] / (BAND * BAND) + 1e-06
    ref = e[:, BAND - 1 :] / (BAND * BAND) + 1e-06
    c = c / (BAND * jnp.sqrt(spec * ref))
    peak = jnp.max(c)
    index = lax.broadcasted_iota(jnp.int32, (WIN, WIN), 0)
    for out, row in ((keep, mine_row), (send, mine_row ^ 1)):
        out[0:1, :] = jnp.sum(jnp.where(index == row, c, 0.0), 0, keepdims=True)
        out[1:2, :] = jnp.full((1, WIN), peak)


def join_kernel(keep, came, rows, peaks):
    core = lax.axis_index("core")
    rows[pl.ds(core, 1), 0, :] = keep[0:1, :]
    rows[pl.ds(1 - core, 1), 0, :] = came[0:1, :]
    peaks[core] = jnp.max(keep[1:2, :])
    peaks[1 - core] = jnp.max(came[1:2, :])


def solution(mesh):
    lines = mesh.shape["slab"] // (COLS * CORES)
    grid = Mesh(
        mesh.devices.reshape(mesh.shape["grp"], lines, COLS, CORES), ("grp", "line", "col", "core")
    )
    slab = ("line", "col", "core")
    vmem = pl.BlockSpec(memory_space=pltpu.VMEM)
    smem = pl.BlockSpec(memory_space=pltpu.SMEM)
    hbm = pl.BlockSpec(memory_space=pltpu.HBM)
    small = pltpu.CompilerParams(vmem_limit_bytes=4 * 1024 * 1024)
    f32, bf16 = jnp.float32, jnp.bfloat16

    def per_device(volume, shift, weight, left, share, center, owner, ref):
        planes, height, width = volume.shape
        row_tab = jnp.asarray(row_table(height))
        col_tab = jnp.asarray(column_table(width))
        tiles = width // LANES
        blocks = planes * VPARTS
        fetched = (shift, weight, center, owner, volume, row_tab, ref)
        keep, send, aux = pl.pallas_call(
            shift_kernel,
            out_shape=[
                jax.ShapeDtypeStruct((tiles * ROWS, LANES), f32),
                jax.ShapeDtypeStruct((tiles * ROWS + 2 * BAND, LANES), f32),
                jax.ShapeDtypeStruct((24, BAND), f32),
            ],
            in_specs=[hbm] * len(fetched),
            out_specs=[vmem] * 3,
            scratch_shapes=[
                pltpu.SMEM(shift.shape, jnp.int32),
                pltpu.SMEM(weight.shape, f32),
                pltpu.SMEM(center.shape, jnp.int32),
                pltpu.SMEM(owner.shape, jnp.int32),
                pltpu.VMEM((blocks, height, width // VPARTS), bf16),
                pltpu.VMEM(row_tab.shape, bf16),
                *[pltpu.VMEM((ROWS, width + 2 * LANES), f32)] * (2 * planes),
                pltpu.SemaphoreType.DMA((7,)),
                pltpu.SemaphoreType.DMA((blocks,)),
            ],
            compiler_params=pltpu.CompilerParams(vmem_limit_bytes=24 * 1024 * 1024),
            name="shift",
        )(*(pltpu.with_memory_space_constraint(a, pltpu.HBM) for a in fetched))
        came = lax.ppermute(send, "core", [(i, (i + 1) % CORES) for i in range(CORES)])
        mixed = pl.pallas_call(
            mix_kernel,
            out_shape=jax.ShapeDtypeStruct(col_tab.shape, bf16),
            in_specs=[vmem] * 4,
            out_specs=vmem,
            compiler_params=pltpu.CompilerParams(vmem_limit_bytes=24 * 1024 * 1024),
            name="mix",
        )(left, share, col_tab, aux)
        packed = pl.pallas_call(
            band_kernel,
            out_shape=jax.ShapeDtypeStruct((HALF, CHUNK, BAND), f32),
            in_specs=[vmem] * 5,
            out_specs=vmem,
            scratch_shapes=[
                pltpu.VMEM((ROWS, width), f32),
                pltpu.VMEM((ROWS, 2 * BAND), f32),
                pltpu.VMEM((2, BAND, BAND), f32),
            ],
            compiler_params=pltpu.CompilerParams(vmem_limit_bytes=24 * 1024 * 1024),
            name="band",
        )(keep, send, came, aux, mixed)
        got = lax.all_to_all(packed, ("line", "col"), 0, 0, tiled=True)
        piece = pl.pallas_call(
            cross_kernel,
            out_shape=jax.ShapeDtypeStruct((HALF, CH_OUT, WIN), f32),
            in_specs=[vmem] * 3,
            out_specs=vmem,
            scratch_shapes=[pltpu.VMEM((16, 2 * BAND), f32)],
            compiler_params=small,
            name="cross",
        )(aux, got, jnp.asarray(window_column_table(width)))
        got = lax.all_to_all(piece, ("line", "col"), 0, 0, tiled=True)
        send, keep = pl.pallas_call(
            window_kernel,
            out_shape=[jax.ShapeDtypeStruct((2, WIN), f32)] * 2,
            in_specs=[vmem] * 2,
            out_specs=[vmem] * 2,
            compiler_params=small,
            name="window",
        )(got, jnp.asarray(window_row_table(height)))
        came = lax.ppermute(send, "core", [(i, (i + 1) % CORES) for i in range(CORES)])
        return pl.pallas_call(
            join_kernel,
            out_shape=[jax.ShapeDtypeStruct((TILTS, 1, WIN), f32), jax.ShapeDtypeStruct((TILTS,), f32)],
            in_specs=[vmem] * 2,
            out_specs=[vmem, smem],
            compiler_params=small,
            name="join",
        )(keep, came)

    placed = (
        P(("grp",) + slab, None, None),
        P("grp", slab),
        P("grp", slab),
        P("grp", None),
        P("grp", None),
        P("grp", None),
        P("grp"),
        P(("grp",) + slab, None, None, None),
    )
    return jax.shard_map(
        per_device,
        mesh=grid,
        in_specs=placed,
        out_specs=(P("grp", slab, None), P("grp")),
        check_vma=False,
    )
```

```python
import numpy as np

import jax
import jax.numpy as jnp
from jax import lax
from jax.experimental import pallas as pl
from jax.experimental.pallas import tpu as pltpu
from jax.sharding import Mesh, PartitionSpec as P
import ml_dtypes

BAND = 128
HALF = BAND // 2
WIN = 128
TILTS = 2
CORES = 2
COLS = 8
ROWS = 136
LANES = 128
VPARTS = 2
CHUNK = 8
CH_OUT = 4


def split(table):
    table = np.asarray(table, np.float32)
    high = table.astype(ml_dtypes.bfloat16)
    low = (table - high.astype(np.float32)).astype(ml_dtypes.bfloat16)
    return high, low


def turns(a, b, length):
    angle = (a[:, None].astype(np.int64) * b[None, :]) % length * (2.0 * np.pi / length)
    return np.cos(angle), np.sin(angle)


def row_table(length):
    c, s = turns(np.arange(HALF + 1), np.arange(length), length)
    out = np.zeros((ROWS, length))
    out[:HALF] = c[:HALF]
    out[HALF] = c[HALF]
    out[HALF + 1 : BAND] = s[1:HALF]
    out[BAND] = s[HALF]
    high, low = split(out)
    return np.concatenate([high, low])


def column_table(length):
    c, s = turns(np.arange(length), np.arange(BAND), length)
    high, low = split(np.concatenate([c, s], 1))
    return np.stack([high, low])


def window_column_table(length):
    c, s = turns(np.arange(BAND), np.arange(WIN) - WIN // 2, length)
    high, low = split(np.concatenate([c, -s], 0))
    return np.stack([high, low])


def window_row_table(length):
    c, s = turns(np.arange(WIN) - WIN // 2, np.arange(HALF + 1), length)
    out = np.zeros((WIN, HALF, CH_OUT))
    out[:, :, 0] = c[:, :HALF]
    out[:, 1:, 1] = -s[:, 1:HALF]
    out[:, 0, 1] = c[:, HALF]
    out[:, 0, 2] = s[:, HALF]
    high, low = split(out.reshape(WIN, HALF * CH_OUT))
    return np.stack([high, low])


def dot(a, b):
    return jnp.dot(a, b, preferred_element_type=jnp.float32)


def halves(x):
    high = x.astype(jnp.bfloat16)
    return high, (x - high.astype(jnp.float32)).astype(jnp.bfloat16)


def shift_kernel(
    h_shift, h_weight, h_center, h_owner, h_volume, h_row, h_ref, keep, send, aux,
    shift, weight, center, owner, volume, row_tab, *rest,
):
    planes, height, width = h_volume.shape
    rpads, sem, vsem = rest[: 2 * planes], rest[-2], rest[-1]
    tiles = width // LANES
    step = 256
    part = height // VPARTS

    def fetch(src, dst, i):
        copy = pltpu.make_async_copy(src, dst, sem.at[i])
        copy.start()
        return copy

    get_row = fetch(h_row, row_tab, 0)
    blocks = []
    for z in range(planes):
        for n in range(VPARTS):
            i = z * VPARTS + n
            cut = pl.ds(n * part, part)
            copy = pltpu.make_async_copy(h_volume.at[z, cut, :], volume.at[z, cut, :], vsem.at[i])
            copy.start()
            blocks.append(copy)
            if i == 0:
                get_center = fetch(h_center, center, 1)
                get_owner = fetch(h_owner, owner, 2)
                get_shift = fetch(h_shift, shift, 3)
                get_weight = fetch(h_weight, weight, 4)
    refs = [fetch(h_ref.at[0, i], send.at[pl.ds(tiles * ROWS + i * BAND, BAND), :], 5 + i) for i in range(2)]

    col = lax.axis_index("col")
    core = lax.axis_index("core")
    get_center.wait()
    get_owner.wait()
    pair = lax.axis_index("line") * COLS + col
    row = lax.broadcasted_iota(jnp.int32, (8, BAND), 0)
    b = lax.broadcasted_iota(jnp.int32, (8, BAND), 1)
    q = jnp.where(row == 0, pair, jnp.where(pair == 0, -HALF, -pair))
    turn = (q * center[core, 0] + b * center[core, 1]) & (width - 1)
    angle = turn.astype(jnp.float32) * (2.0 * np.pi / width)
    aux[:8, :] = jnp.cos(angle)
    aux[8:16, :] = jnp.sin(angle)
    who = pair * CORES + jnp.where(row == 0, core, 1 - core)
    aux[16:, :] = jnp.where(who == owner[core], 1.0, 0.0)
    get_shift.wait()
    get_weight.wait()
    get_row.wait()

    lane = lax.broadcasted_iota(jnp.int32, (8, LANES), 1)
    first = lane == 0

    def transform(z):
        near = rpads[2 * z]
        for copy in blocks[z * VPARTS : (z + 1) * VPARTS]:
            copy.wait()
        for n in range(0, width, step):
            r = dot(row_tab[...], volume[z, :, n : n + step])
            near[:, n : n + step] = r[:ROWS] + r[ROWS:]

    def move(z):
        near, far = rpads[2 * z], rpads[2 * z + 1]
        for g in range(ROWS // 8):
            rows = slice(g * 8, g * 8 + 8)
            turned = [pltpu.roll(near[rows, LANES * j : LANES * (j + 1)], 1, 1) for j in range(tiles)]
            for j in range(tiles + 1):
                left = turned[j - 1] if j else 0.0
                here = turned[j] if j < tiles else 0.0
                far[rows, LANES * j : LANES * (j + 1)] = jnp.where(first, left, here)
        for t, out in ((1 - core, send), (core, keep)):
            w = weight[t, z]
            s = shift[t, z]
            turn = jnp.where(s < 0, s + LANES, s)
            before = lane < jnp.where(s < 0, 0, s)
            after = lane >= jnp.where(s < 0, s + LANES, LANES)
            for g in range(ROWS // 8):
                rows = slice(g * 8, g * 8 + 8)
                turned = []
                for j in range(tiles + 1):
                    at = slice(LANES * j, LANES * (j + 1))
                    mixed = w * far[rows, at]
                    if j < tiles:
                        mixed = (1.0 - w) * near[rows, at] + mixed
                    turned.append(pltpu.roll(mixed, turn, 1))
                for j in range(tiles):
                    left = turned[j - 1] if j else 0.0
                    term = jnp.where(before, left, jnp.where(after, turned[j + 1], turned[j]))
                    at = j * ROWS + g * 8
                    out[at : at + 8, :] = term if z == 0 else out[at : at + 8, :] + term

    transform(0)
    for z in range(planes):
        if z + 1 < planes:
            transform(z + 1)
        move(z)
    for copy in refs:
        copy.wait()


def mix_kernel(left, share, col_tab, after, out):
    width = left.shape[1]
    step = 256
    core = lax.axis_index("core")
    at = left[pl.ds(core, 1), :]
    w = share[pl.ds(core, 1), :]
    near_high, near_low = halves(1.0 - w)
    far_high, far_low = halves(w)
    none = jnp.zeros((step, width), jnp.bfloat16)
    x = lax.broadcasted_iota(jnp.int32, (step, width), 0).astype(jnp.float32).astype(jnp.bfloat16)
    for n in range(0, width, step):

        def is_at(place):
            inside = (place >= 0) & (place < step)
            return x == jnp.where(inside, place, -8).astype(jnp.float32).astype(jnp.bfloat16)

        near, far = is_at(at - n), is_at(at + 1 - n)
        high = jnp.where(near, near_high, jnp.where(far, far_high, none))
        low = jnp.where(near, near_low, jnp.where(far, far_low, none))
        y = dot(high, col_tab[0]) + dot(low, col_tab[0]) + dot(high, col_tab[1])
        high, low = halves(y)
        out[0, n : n + step, :] = high
        out[1, n : n + step, :] = low


def band_kernel(keep, sent, came, aux, mixed, out, sums, band, own):
    tiles = keep.shape[0] // ROWS
    for j in range(tiles):
        rows = slice(j * ROWS, (j + 1) * ROWS)
        sums[:, j * LANES : (j + 1) * LANES] = keep[rows, :] + came[rows, :]
    high, low = halves(sums[...])
    band[...] = dot(high, mixed[0]) + dot(low, mixed[0]) + dot(high, mixed[1])
    row = band[HALF : HALF + 1, :]
    last = band[BAND : BAND + 1, :]
    band[HALF : HALF + 1, :BAND] = row[:, :BAND] + last[:, BAND:]
    band[HALF : HALF + 1, BAND:] = row[:, BAND:] - last[:, :BAND]
    mine = aux[16:17, :] > 0.5
    theirs = aux[17:18, :] > 0.5
    for i in range(2):
        at = slice(tiles * ROWS + i * BAND, tiles * ROWS + (i + 1) * BAND)
        own[i] = jnp.where(mine, sent[at, :], jnp.where(theirs, came[at, :], 0.0))
    for p in range(HALF):
        minus = HALF - p if p else 0
        for i in range(2):
            out[p, i : i + 1, :] = band[p : p + 1, i * BAND : (i + 1) * BAND]
            out[p, 2 + i : 3 + i, :] = band[HALF + p : HALF + p + 1, i * BAND : (i + 1) * BAND]
            out[p, 4 + i : 5 + i, :] = own[i, HALF + p : HALF + p + 1, :]
            out[p, 6 + i : 7 + i, :] = own[i, minus : minus + 1, :]


def cross_kernel(aux, got, tab, out, lhs):
    n = got.shape[0]
    parts = [got[i] for i in range(8)]
    for i in range(8, n):
        parts[i % 8] = parts[i % 8] + got[i]
    while len(parts) > 1:
        parts = [parts[i] + parts[i + 1] for i in range(0, len(parts), 2)]
    total = parts[0]
    pair = lax.axis_index("line") * COLS + lax.axis_index("col")
    zero = lax.broadcasted_iota(jnp.int32, (1, BAND), 1) * 0 + pair == 0
    cc, cs, sc, ss, *refs = (total[i : i + 1, :] for i in range(8))
    plus = (jnp.where(zero, cc, cc - ss), -jnp.where(zero, cs, cs + sc))
    minus = (jnp.where(zero, sc, cc + ss), -jnp.where(zero, ss, cs - sc))
    crossed = []
    e_spec = e_ref = 0.0
    for i, ((sr, si), (rr, ri)) in enumerate(((plus, refs[:2]), (minus, refs[2:]))):
        cr = sr * rr + si * ri
        ci = si * rr - sr * ri
        e_spec = e_spec + sr * sr + si * si
        e_ref = e_ref + rr * rr + ri * ri
        co = aux[i : i + 1, :]
        sn = aux[8 + i : 9 + i, :]
        crossed.append((cr * co - ci * sn, cr * sn + ci * co))
    (pr, pi), (mr, mi) = crossed
    lhs[...] = jnp.zeros(lhs.shape, jnp.float32)
    lhs[0:1, :BAND] = jnp.where(zero, pr, pr + mr)
    lhs[0:1, BAND:] = jnp.where(zero, pi, pi + mi)
    lhs[1:2, :BAND] = jnp.where(zero, mr, pi - mi)
    lhs[1:2, BAND:] = jnp.where(zero, mi, mr - pr)
    lhs[2:3, :BAND] = mi
    lhs[2:3, BAND:] = -mr
    high, low = halves(lhs[...])
    h = dot(high, tab[0]) + dot(low, tab[0]) + dot(high, tab[1])
    lane = lax.broadcasted_iota(jnp.int32, (1, BAND), 1)
    e_spec = jnp.sum(e_spec, 1, keepdims=True)
    e_ref = jnp.sum(e_ref, 1, keepdims=True)
    lhs[:8, :BAND] = h[:8]
    lhs[3:4, :BAND] = jnp.where(lane < BAND // 2, e_spec, e_ref)
    done = lhs[:CH_OUT, :BAND]
    for d in range(out.shape[0]):
        out[d] = done


def window_kernel(got, tab, send, keep):
    n = got.shape[0]
    mine_row = (lax.axis_index("line") * COLS + lax.axis_index("col")) * CORES + lax.axis_index("core")
    high, low = halves(got[...].reshape(n * CH_OUT, WIN))
    c = dot(tab[0], high) + dot(tab[0], low) + dot(tab[1], high)
    e = jnp.sum(got[:, CH_OUT - 1, :], 0, keepdims=True)
    spec = e[:, :1] / (BAND * BAND) + 1e-06
    ref = e[:, BAND - 1 :] / (BAND * BAND) + 1e-06
    c = c / (BAND * jnp.sqrt(spec * ref))
    peak = jnp.max(c)
    index = lax.broadcasted_iota(jnp.int32, (WIN, WIN), 0)
    for out, row in ((keep, mine_row), (send, mine_row ^ 1)):
        out[0:1, :] = jnp.sum(jnp.where(index == row, c, 0.0), 0, keepdims=True)
        out[1:2, :] = jnp.full((1, WIN), peak)


def join_kernel(keep, came, rows, peaks):
    core = lax.axis_index("core")
    rows[pl.ds(core, 1), 0, :] = keep[0:1, :]
    rows[pl.ds(1 - core, 1), 0, :] = came[0:1, :]
    peaks[core] = jnp.max(keep[1:2, :])
    peaks[1 - core] = jnp.max(came[1:2, :])


def solution(mesh):
    lines = mesh.shape["slab"] // (COLS * CORES)
    grid = Mesh(
        mesh.devices.reshape(mesh.shape["grp"], lines, COLS, CORES), ("grp", "line", "col", "core")
    )
    slab = ("line", "col", "core")
    vmem = pl.BlockSpec(memory_space=pltpu.VMEM)
    smem = pl.BlockSpec(memory_space=pltpu.SMEM)
    hbm = pl.BlockSpec(memory_space=pltpu.HBM)
    small = pltpu.CompilerParams(vmem_limit_bytes=4 * 1024 * 1024)
    f32, bf16 = jnp.float32, jnp.bfloat16

    def per_device(volume, shift, weight, left, share, center, owner, ref):
        planes, height, width = volume.shape
        row_tab = jnp.asarray(row_table(height))
        col_tab = jnp.asarray(column_table(width))
        tiles = width // LANES
        blocks = planes * VPARTS
        fetched = (shift, weight, center, owner, volume, row_tab, ref)
        keep, send, aux = pl.pallas_call(
            shift_kernel,
            out_shape=[
                jax.ShapeDtypeStruct((tiles * ROWS, LANES), f32),
                jax.ShapeDtypeStruct((tiles * ROWS + 2 * BAND, LANES), f32),
                jax.ShapeDtypeStruct((24, BAND), f32),
            ],
            in_specs=[hbm] * len(fetched),
            out_specs=[vmem] * 3,
            scratch_shapes=[
                pltpu.SMEM(shift.shape, jnp.int32),
                pltpu.SMEM(weight.shape, f32),
                pltpu.SMEM(center.shape, jnp.int32),
                pltpu.SMEM(owner.shape, jnp.int32),
                pltpu.VMEM(volume.shape, bf16),
                pltpu.VMEM(row_tab.shape, bf16),
                *[pltpu.VMEM((ROWS, width + LANES), f32)] * (2 * planes),
                pltpu.SemaphoreType.DMA((7,)),
                pltpu.SemaphoreType.DMA((blocks,)),
            ],
            compiler_params=pltpu.CompilerParams(vmem_limit_bytes=24 * 1024 * 1024),
            name="shift",
        )(*(pltpu.with_memory_space_constraint(a, pltpu.HBM) for a in fetched))
        came = lax.ppermute(send, "core", [(i, (i + 1) % CORES) for i in range(CORES)])
        mixed = pl.pallas_call(
            mix_kernel,
            out_shape=jax.ShapeDtypeStruct(col_tab.shape, bf16),
            in_specs=[vmem] * 4,
            out_specs=vmem,
            compiler_params=pltpu.CompilerParams(vmem_limit_bytes=24 * 1024 * 1024),
            name="mix",
        )(left, share, col_tab, aux)
        packed = pl.pallas_call(
            band_kernel,
            out_shape=jax.ShapeDtypeStruct((HALF, CHUNK, BAND), f32),
            in_specs=[vmem] * 5,
            out_specs=vmem,
            scratch_shapes=[
                pltpu.VMEM((ROWS, width), f32),
                pltpu.VMEM((ROWS, 2 * BAND), f32),
                pltpu.VMEM((2, BAND, BAND), f32),
            ],
            compiler_params=pltpu.CompilerParams(vmem_limit_bytes=24 * 1024 * 1024),
            name="band",
        )(keep, send, came, aux, mixed)
        got = lax.all_to_all(packed, ("line", "col"), 0, 0, tiled=True)
        piece = pl.pallas_call(
            cross_kernel,
            out_shape=jax.ShapeDtypeStruct((HALF, CH_OUT, WIN), f32),
            in_specs=[vmem] * 3,
            out_specs=vmem,
            scratch_shapes=[pltpu.VMEM((16, 2 * BAND), f32)],
            compiler_params=small,
            name="cross",
        )(aux, got, jnp.asarray(window_column_table(width)))
        got = lax.all_to_all(piece, ("line", "col"), 0, 0, tiled=True)
        send, keep = pl.pallas_call(
            window_kernel,
            out_shape=[jax.ShapeDtypeStruct((2, WIN), f32)] * 2,
            in_specs=[vmem] * 2,
            out_specs=[vmem] * 2,
            compiler_params=small,
            name="window",
        )(got, jnp.asarray(window_row_table(height)))
        came = lax.ppermute(send, "core", [(i, (i + 1) % CORES) for i in range(CORES)])
        return pl.pallas_call(
            join_kernel,
            out_shape=[jax.ShapeDtypeStruct((TILTS, 1, WIN), f32), jax.ShapeDtypeStruct((TILTS,), f32)],
            in_specs=[vmem] * 2,
            out_specs=[vmem, smem],
            compiler_params=small,
            name="join",
        )(keep, came)

    placed = (
        P(("grp",) + slab, None, None),
        P("grp", slab),
        P("grp", slab),
        P("grp", None),
        P("grp", None),
        P("grp", None),
        P("grp"),
        P(("grp",) + slab, None, None, None),
    )
    return jax.shard_map(
        per_device,
        mesh=grid,
        in_specs=placed,
        out_specs=(P("grp", slab, None), P("grp")),
        check_vma=False,
    )
```

```python
import numpy as np

import jax
import jax.numpy as jnp
from jax import lax
from jax.experimental import pallas as pl
from jax.experimental.pallas import tpu as pltpu
from jax.sharding import Mesh, PartitionSpec as P
import ml_dtypes

BAND = 128
HALF = BAND // 2
WIN = 128
TILTS = 2
CORES = 2
COLS = 8
ROWS = 136
LANES = 128
VPARTS = 2
CHUNK = 8
CH_OUT = 4


def split(table):
    table = np.asarray(table, np.float32)
    high = table.astype(ml_dtypes.bfloat16)
    low = (table - high.astype(np.float32)).astype(ml_dtypes.bfloat16)
    return high, low


def turns(a, b, length):
    angle = (a[:, None].astype(np.int64) * b[None, :]) % length * (2.0 * np.pi / length)
    return np.cos(angle), np.sin(angle)


def row_table(length):
    c, s = turns(np.arange(HALF + 1), np.arange(length), length)
    out = np.zeros((ROWS, length))
    out[:HALF] = c[:HALF]
    out[HALF] = c[HALF]
    out[HALF + 1 : BAND] = s[1:HALF]
    out[BAND] = s[HALF]
    high, low = split(out)
    return np.concatenate([high, low])


def column_table(length):
    c, s = turns(np.arange(length), np.arange(BAND), length)
    high, low = split(np.concatenate([c, s], 1))
    return np.stack([high, low])


def window_column_table(length):
    c, s = turns(np.arange(BAND), np.arange(WIN) - WIN // 2, length)
    high, low = split(np.concatenate([c, -s], 0))
    return np.stack([high, low])


def window_row_table(length):
    c, s = turns(np.arange(WIN) - WIN // 2, np.arange(HALF + 1), length)
    out = np.zeros((WIN, HALF, CH_OUT))
    out[:, :, 0] = c[:, :HALF]
    out[:, 1:, 1] = -s[:, 1:HALF]
    out[:, 0, 1] = c[:, HALF]
    out[:, 0, 2] = s[:, HALF]
    high, low = split(out.reshape(WIN, HALF * CH_OUT))
    return np.stack([high, low])


def dot(a, b):
    return jnp.dot(a, b, preferred_element_type=jnp.float32)


def halves(x):
    high = x.astype(jnp.bfloat16)
    return high, (x - high.astype(jnp.float32)).astype(jnp.bfloat16)


def shift_kernel(
    h_shift, h_weight, h_center, h_owner, h_volume, h_row, h_ref, keep, send, aux,
    shift, weight, center, owner, volume, row_tab, *rest,
):
    planes, height, width = h_volume.shape
    rpads, sem, vsem = rest[: 2 * planes], rest[-2], rest[-1]
    tiles = width // LANES
    step = 256
    part = height // VPARTS

    def fetch(src, dst, i):
        copy = pltpu.make_async_copy(src, dst, sem.at[i])
        copy.start()
        return copy

    get_row = fetch(h_row, row_tab, 0)
    blocks = []
    for z in range(planes):
        for n in range(VPARTS):
            i = z * VPARTS + n
            cut = pl.ds(n * part, part)
            copy = pltpu.make_async_copy(h_volume.at[z, cut, :], volume.at[z, cut, :], vsem.at[i])
            copy.start()
            blocks.append(copy)
            if i == 0:
                get_center = fetch(h_center, center, 1)
                get_owner = fetch(h_owner, owner, 2)
                get_shift = fetch(h_shift, shift, 3)
                get_weight = fetch(h_weight, weight, 4)
    refs = [fetch(h_ref.at[0, i], send.at[pl.ds(tiles * ROWS + i * BAND, BAND), :], 5 + i) for i in range(2)]

    col = lax.axis_index("col")
    core = lax.axis_index("core")
    get_center.wait()
    get_owner.wait()
    pair = lax.axis_index("line") * COLS + col
    row = lax.broadcasted_iota(jnp.int32, (8, BAND), 0)
    b = lax.broadcasted_iota(jnp.int32, (8, BAND), 1)
    q = jnp.where(row == 0, pair, jnp.where(pair == 0, -HALF, -pair))
    turn = (q * center[core, 0] + b * center[core, 1]) & (width - 1)
    angle = turn.astype(jnp.float32) * (2.0 * np.pi / width)
    aux[:8, :] = jnp.cos(angle)
    aux[8:16, :] = jnp.sin(angle)
    who = pair * CORES + jnp.where(row == 0, core, 1 - core)
    aux[16:, :] = jnp.where(who == owner[core], 1.0, 0.0)
    get_shift.wait()
    get_weight.wait()
    get_row.wait()

    lane = lax.broadcasted_iota(jnp.int32, (8, LANES), 1)
    first = lane == 0

    def transform(z):
        near = rpads[2 * z]
        mine = blocks[z * VPARTS : (z + 1) * VPARTS]
        cuts = [slice(n * part, (n + 1) * part) for n in range(VPARTS)]
        if z:
            for copy in mine:
                copy.wait()
            cuts = [slice(0, height)]
        for i, cut in enumerate(cuts):
            if not z:
                mine[i].wait()
            for n in range(0, width, step):
                r = dot(row_tab[:, cut], volume[z, cut, n : n + step])
                r = r[:ROWS] + r[ROWS:]
                near[:, n : n + step] = near[:, n : n + step] + r if i else r

    def move(z):
        near, far = rpads[2 * z], rpads[2 * z + 1]
        for g in range(ROWS // 8):
            rows = slice(g * 8, g * 8 + 8)
            turned = [pltpu.roll(near[rows, LANES * j : LANES * (j + 1)], 1, 1) for j in range(tiles)]
            for j in range(tiles + 1):
                left = turned[j - 1] if j else 0.0
                here = turned[j] if j < tiles else 0.0
                far[rows, LANES * j : LANES * (j + 1)] = jnp.where(first, left, here)
        for t, out in ((1 - core, send), (core, keep)):
            w = weight[t, z]
            s = shift[t, z]
            turn = jnp.where(s < 0, s + LANES, s)
            before = lane < jnp.where(s < 0, 0, s)
            after = lane >= jnp.where(s < 0, s + LANES, LANES)
            for g in range(ROWS // 8):
                rows = slice(g * 8, g * 8 + 8)
                turned = []
                for j in range(tiles + 1):
                    at = slice(LANES * j, LANES * (j + 1))
                    mixed = w * far[rows, at]
                    if j < tiles:
                        mixed = (1.0 - w) * near[rows, at] + mixed
                    turned.append(pltpu.roll(mixed, turn, 1))
                for j in range(tiles):
                    left = turned[j - 1] if j else 0.0
                    term = jnp.where(before, left, jnp.where(after, turned[j + 1], turned[j]))
                    at = j * ROWS + g * 8
                    out[at : at + 8, :] = term if z == 0 else out[at : at + 8, :] + term

    transform(0)
    for z in range(planes):
        if z + 1 < planes:
            transform(z + 1)
        move(z)
    for copy in refs:
        copy.wait()


def mix_kernel(left, share, col_tab, after, out):
    width = left.shape[1]
    step = 256
    core = lax.axis_index("core")
    at = left[pl.ds(core, 1), :]
    w = share[pl.ds(core, 1), :]
    near_high, near_low = halves(1.0 - w)
    far_high, far_low = halves(w)
    none = jnp.zeros((step, width), jnp.bfloat16)
    x = lax.broadcasted_iota(jnp.int32, (step, width), 0).astype(jnp.float32).astype(jnp.bfloat16)
    for n in range(0, width, step):

        def is_at(place):
            inside = (place >= 0) & (place < step)
            return x == jnp.where(inside, place, -8).astype(jnp.float32).astype(jnp.bfloat16)

        near, far = is_at(at - n), is_at(at + 1 - n)
        high = jnp.where(near, near_high, jnp.where(far, far_high, none))
        low = jnp.where(near, near_low, jnp.where(far, far_low, none))
        y = dot(high, col_tab[0]) + dot(low, col_tab[0]) + dot(high, col_tab[1])
        high, low = halves(y)
        out[0, n : n + step, :] = high
        out[1, n : n + step, :] = low


def band_kernel(keep, sent, came, aux, mixed, out, sums, band, own):
    tiles = keep.shape[0] // ROWS
    for j in range(tiles):
        rows = slice(j * ROWS, (j + 1) * ROWS)
        sums[:, j * LANES : (j + 1) * LANES] = keep[rows, :] + came[rows, :]
    high, low = halves(sums[...])
    band[...] = dot(high, mixed[0]) + dot(low, mixed[0]) + dot(high, mixed[1])
    row = band[HALF : HALF + 1, :]
    last = band[BAND : BAND + 1, :]
    band[HALF : HALF + 1, :BAND] = row[:, :BAND] + last[:, BAND:]
    band[HALF : HALF + 1, BAND:] = row[:, BAND:] - last[:, :BAND]
    mine = aux[16:17, :] > 0.5
    theirs = aux[17:18, :] > 0.5
    for i in range(2):
        at = slice(tiles * ROWS + i * BAND, tiles * ROWS + (i + 1) * BAND)
        own[i] = jnp.where(mine, sent[at, :], jnp.where(theirs, came[at, :], 0.0))
    for p in range(HALF):
        minus = HALF - p if p else 0
        for i in range(2):
            out[p, i : i + 1, :] = band[p : p + 1, i * BAND : (i + 1) * BAND]
            out[p, 2 + i : 3 + i, :] = band[HALF + p : HALF + p + 1, i * BAND : (i + 1) * BAND]
            out[p, 4 + i : 5 + i, :] = own[i, HALF + p : HALF + p + 1, :]
            out[p, 6 + i : 7 + i, :] = own[i, minus : minus + 1, :]


def cross_kernel(aux, got, tab, out, lhs):
    n = got.shape[0]
    parts = [got[i] for i in range(8)]
    for i in range(8, n):
        parts[i % 8] = parts[i % 8] + got[i]
    while len(parts) > 1:
        parts = [parts[i] + parts[i + 1] for i in range(0, len(parts), 2)]
    total = parts[0]
    pair = lax.axis_index("line") * COLS + lax.axis_index("col")
    zero = lax.broadcasted_iota(jnp.int32, (1, BAND), 1) * 0 + pair == 0
    cc, cs, sc, ss, *refs = (total[i : i + 1, :] for i in range(8))
    plus = (jnp.where(zero, cc, cc - ss), -jnp.where(zero, cs, cs + sc))
    minus = (jnp.where(zero, sc, cc + ss), -jnp.where(zero, ss, cs - sc))
    crossed = []
    e_spec = e_ref = 0.0
    for i, ((sr, si), (rr, ri)) in enumerate(((plus, refs[:2]), (minus, refs[2:]))):
        cr = sr * rr + si * ri
        ci = si * rr - sr * ri
        e_spec = e_spec + sr * sr + si * si
        e_ref = e_ref + rr * rr + ri * ri
        co = aux[i : i + 1, :]
        sn = aux[8 + i : 9 + i, :]
        crossed.append((cr * co - ci * sn, cr * sn + ci * co))
    (pr, pi), (mr, mi) = crossed
    lhs[...] = jnp.zeros(lhs.shape, jnp.float32)
    lhs[0:1, :BAND] = jnp.where(zero, pr, pr + mr)
    lhs[0:1, BAND:] = jnp.where(zero, pi, pi + mi)
    lhs[1:2, :BAND] = jnp.where(zero, mr, pi - mi)
    lhs[1:2, BAND:] = jnp.where(zero, mi, mr - pr)
    lhs[2:3, :BAND] = mi
    lhs[2:3, BAND:] = -mr
    high, low = halves(lhs[...])
    h = dot(high, tab[0]) + dot(low, tab[0]) + dot(high, tab[1])
    lane = lax.broadcasted_iota(jnp.int32, (1, BAND), 1)
    e_spec = jnp.sum(e_spec, 1, keepdims=True)
    e_ref = jnp.sum(e_ref, 1, keepdims=True)
    lhs[:8, :BAND] = h[:8]
    lhs[3:4, :BAND] = jnp.where(lane < BAND // 2, e_spec, e_ref)
    done = lhs[:CH_OUT, :BAND]
    for d in range(out.shape[0]):
        out[d] = done


def window_kernel(got, tab, send, keep):
    n = got.shape[0]
    mine_row = (lax.axis_index("line") * COLS + lax.axis_index("col")) * CORES + lax.axis_index("core")
    high, low = halves(got[...].reshape(n * CH_OUT, WIN))
    c = dot(tab[0], high) + dot(tab[0], low) + dot(tab[1], high)
    e = jnp.sum(got[:, CH_OUT - 1, :], 0, keepdims=True)
    spec = e[:, :1] / (BAND * BAND) + 1e-06
    ref = e[:, BAND - 1 :] / (BAND * BAND) + 1e-06
    c = c / (BAND * jnp.sqrt(spec * ref))
    peak = jnp.max(c)
    index = lax.broadcasted_iota(jnp.int32, (WIN, WIN), 0)
    for out, row in ((keep, mine_row), (send, mine_row ^ 1)):
        out[0:1, :] = jnp.sum(jnp.where(index == row, c, 0.0), 0, keepdims=True)
        out[1:2, :] = jnp.full((1, WIN), peak)


def join_kernel(keep, came, rows, peaks):
    core = lax.axis_index("core")
    rows[pl.ds(core, 1), 0, :] = keep[0:1, :]
    rows[pl.ds(1 - core, 1), 0, :] = came[0:1, :]
    peaks[core] = keep[1, 0]
    peaks[1 - core] = came[1, 0]


def solution(mesh):
    lines = mesh.shape["slab"] // (COLS * CORES)
    grid = Mesh(
        mesh.devices.reshape(mesh.shape["grp"], lines, COLS, CORES), ("grp", "line", "col", "core")
    )
    slab = ("line", "col", "core")
    vmem = pl.BlockSpec(memory_space=pltpu.VMEM)
    smem = pl.BlockSpec(memory_space=pltpu.SMEM)
    hbm = pl.BlockSpec(memory_space=pltpu.HBM)
    small = pltpu.CompilerParams(vmem_limit_bytes=4 * 1024 * 1024)
    f32, bf16 = jnp.float32, jnp.bfloat16

    def per_device(volume, shift, weight, left, share, center, owner, ref):
        planes, height, width = volume.shape
        row_tab = jnp.asarray(row_table(height))
        col_tab = jnp.asarray(column_table(width))
        tiles = width // LANES
        blocks = planes * VPARTS
        fetched = (shift, weight, center, owner, volume, row_tab, ref)
        keep, send, aux = pl.pallas_call(
            shift_kernel,
            out_shape=[
                jax.ShapeDtypeStruct((tiles * ROWS, LANES), f32),
                jax.ShapeDtypeStruct((tiles * ROWS + 2 * BAND, LANES), f32),
                jax.ShapeDtypeStruct((24, BAND), f32),
            ],
            in_specs=[hbm] * len(fetched),
            out_specs=[vmem] * 3,
            scratch_shapes=[
                pltpu.SMEM(shift.shape, jnp.int32),
                pltpu.SMEM(weight.shape, f32),
                pltpu.SMEM(center.shape, jnp.int32),
                pltpu.SMEM(owner.shape, jnp.int32),
                pltpu.VMEM(volume.shape, bf16),
                pltpu.VMEM(row_tab.shape, bf16),
                *[pltpu.VMEM((ROWS, width + LANES), f32)] * (2 * planes),
                pltpu.SemaphoreType.DMA((7,)),
                pltpu.SemaphoreType.DMA((blocks,)),
            ],
            compiler_params=pltpu.CompilerParams(vmem_limit_bytes=24 * 1024 * 1024),
            name="shift",
        )(*(pltpu.with_memory_space_constraint(a, pltpu.HBM) for a in fetched))
        came = lax.ppermute(send, "core", [(i, (i + 1) % CORES) for i in range(CORES)])
        mixed = pl.pallas_call(
            mix_kernel,
            out_shape=jax.ShapeDtypeStruct(col_tab.shape, bf16),
            in_specs=[vmem] * 4,
            out_specs=vmem,
            compiler_params=pltpu.CompilerParams(vmem_limit_bytes=24 * 1024 * 1024),
            name="mix",
        )(left, share, col_tab, aux)
        packed = pl.pallas_call(
            band_kernel,
            out_shape=jax.ShapeDtypeStruct((HALF, CHUNK, BAND), f32),
            in_specs=[vmem] * 5,
            out_specs=vmem,
            scratch_shapes=[
                pltpu.VMEM((ROWS, width), f32),
                pltpu.VMEM((ROWS, 2 * BAND), f32),
                pltpu.VMEM((2, BAND, BAND), f32),
            ],
            compiler_params=pltpu.CompilerParams(vmem_limit_bytes=24 * 1024 * 1024),
            name="band",
        )(keep, send, came, aux, mixed)
        got = lax.all_to_all(packed, ("line", "col"), 0, 0, tiled=True)
        piece = pl.pallas_call(
            cross_kernel,
            out_shape=jax.ShapeDtypeStruct((HALF, CH_OUT, WIN), f32),
            in_specs=[vmem] * 3,
            out_specs=vmem,
            scratch_shapes=[pltpu.VMEM((16, 2 * BAND), f32)],
            compiler_params=small,
            name="cross",
        )(aux, got, jnp.asarray(window_column_table(width)))
        got = lax.all_to_all(piece, ("line", "col"), 0, 0, tiled=True)
        send, keep = pl.pallas_call(
            window_kernel,
            out_shape=[jax.ShapeDtypeStruct((2, WIN), f32)] * 2,
            in_specs=[vmem] * 2,
            out_specs=[vmem] * 2,
            compiler_params=small,
            name="window",
        )(got, jnp.asarray(window_row_table(height)))
        came = lax.ppermute(send, "core", [(i, (i + 1) % CORES) for i in range(CORES)])
        return pl.pallas_call(
            join_kernel,
            out_shape=[jax.ShapeDtypeStruct((TILTS, 1, WIN), f32), jax.ShapeDtypeStruct((TILTS,), f32)],
            in_specs=[vmem] * 2,
            out_specs=[vmem, smem],
            compiler_params=small,
            name="join",
        )(keep, came)

    placed = (
        P(("grp",) + slab, None, None),
        P("grp", slab),
        P("grp", slab),
        P("grp", None),
        P("grp", None),
        P("grp", None),
        P("grp"),
        P(("grp",) + slab, None, None, None),
    )
    return jax.shard_map(
        per_device,
        mesh=grid,
        in_specs=placed,
        out_specs=(P("grp", slab, None), P("grp")),
        check_vma=False,
    )
```
